256 devices in a mesh: depth: 32 (over z, y), batch: 8 (over x, core).
Axes of the slice: x: 4, y: 4, z: 8, core: 2. Of those that a mesh axis runs over, the one named last changes fastest.
Arguments:
- iterate: float32 [32, 16, 16, 16, 256], P('depth', 'batch'), may hold values from -70 to 70
- weights: bfloat16 [128, 3, 3, 256, 256], P('depth'), may hold values from -0.125 to 0.125
- norm_scale: float32 [128, 256], P('depth'), may hold values from 0.5 to 2
- norm_shift: float32 [128, 256], P('depth'), may hold values from -3 to 3
Outputs:
- block_ends: float32 [32, 16, 16, 16, 256], P('depth', 'batch')
The draws below stay inside these ranges and needn't reach their ends.
All inputs are finite; a program needn't handle non-finite values.
Results may differ from the reference program's by a relative error of at most 0.0018.
Values sent between devices are 32-bit elements; how exact they have to be, the bound alone decides.
A program may use at most 64 MiB of HBM per device.

```python
import math
import jax
import jax.numpy as jnp
from jax import lax

C = 256
SIDE = 16
SAMPLES = 2
BLOCKS = 32
LAYERS = 128
BATCH = 16


def draw_iterate(key, part):
    key_list = jax.random.split(key, 7)
    array_shape = (BLOCKS, BATCH, SIDE, SIDE, C)
    raw_values = jnp.clip(jax.random.normal(key_list[0], array_shape, jnp.float32), -4.0, 4.0)
    pixel_low = math.log(0.3)
    pixel_scale = jnp.exp(jax.random.uniform(key_list[1], (BLOCKS, BATCH, SIDE, SIDE, 1), jnp.float32, pixel_low, math.log(3.0)))
    channel_scale = jnp.exp(jax.random.uniform(key_list[2], (BLOCKS, 1, 1, 1, C), jnp.float32, math.log(0.3), math.log(3.0)))
    groups = BATCH // SAMPLES
    magnitude = jax.random.uniform(key_list[5], (groups, C), jnp.float32, 2.0, 4.0)
    signs = jnp.where(jax.random.bernoulli(key_list[6], 0.5, (groups, C)), 1.0, -1.0).astype(jnp.float32)
    owner = jnp.arange(BATCH) // SAMPLES
    shifted = (magnitude * signs)[owner].reshape(1, BATCH, 1, 1, C)
    fraction = jnp.arange(BATCH, dtype=jnp.float32) / max(BATCH - 1, 1)
    sample_scale = jnp.exp(math.log(3.0) * (fraction - 0.5)).reshape(1, BATCH, 1, 1, 1)
    return ((raw_values * pixel_scale * channel_scale + shifted) * sample_scale).astype(jnp.float32)


def level_of(rng, dims, shards, smallest, top_value):
    def one(position, parts):
        heights = jax.random.uniform(jax.random.fold_in(jax.random.fold_in(rng, 6), position), (parts,), jnp.float32, smallest / len(shards), top_value / len(shards))
        return jnp.repeat(jnp.exp(heights), dims[position] // parts).reshape((-1,) + (1,) * (len(dims) - position - 1))

    level = one(*shards[0])
    for cut in shards[1:]:
        level = level * one(*cut)
    return level


def scatter_about(stream_key, dims, scale, most, pieces=(), held_as=jnp.bfloat16):
    level = level_of(stream_key, dims, pieces, -0.22, 0.18) if pieces else 1.0
    array = jax.random.normal(stream_key, dims, jnp.float32) * scale * level
    return jnp.minimum(jnp.maximum(array, -most), most).astype(held_as)


def setup_inputs(seed: int = 0) -> dict:
    keys = jax.random.split(jax.random.key(seed), 5)
    iterate = draw_iterate(jax.random.fold_in(keys[4], 71), 0)
    weights = scatter_about(keys[1], (LAYERS, 3, 3, C, C), (9 * C) ** -0.5, 0.125, ((0, 32),))
    norm_scale = jnp.clip(jnp.exp(math.log(2.0) - 1.3862944 * jax.random.uniform(keys[2], (LAYERS, C), jnp.float32) ** level_of(keys[2], (LAYERS, C), ((0, 32),), -0.2, 0.2)), 0.5, 2.0)
    norm_shift = scatter_about(keys[3], (LAYERS, C), 0.5, 3.0, ((0, 32),), jnp.float32)
    return {"iterate": iterate, "weights": weights, "norm_scale": norm_scale, "norm_shift": norm_shift}


fine_step = 0.125
coarse_step = 0.5
epsilon = 1e-05

def convolve(activated, kernel):
    return lax.conv_general_dilated(activated.astype(jnp.float32), kernel.astype(jnp.float32), (1, 1), 'SAME', dimension_numbers=('NHWC', 'HWIO', 'NHWC'), precision=lax.Precision.HIGHEST, preferred_element_type=jnp.float32)

def activate(current, gain_row, offset, center, inverse):
    return jax.nn.relu(gain_row * (current - center) * inverse + offset).astype(jnp.bfloat16)

def fine_layer(current, kernel, gain_row, offset):
    entries = current.shape[0] * current.shape[1] * current.shape[2]
    center = lax.optimization_barrier(jnp.sum(current, axis=(0, 1, 2))) / entries
    inverse = lax.rsqrt(lax.optimization_barrier(jnp.sum(current * current, axis=(0, 1, 2))) / entries - center * center + epsilon)
    activated = activate(current, gain_row, offset, center, inverse)
    return (current + fine_step * convolve(activated, kernel), center, inverse)

def block_map(current, kernels, gains, offsets):
    first_center = None
    first_inverse = None
    for number in range(4):
        current, center, inverse = fine_layer(current, kernels[number], gains[number], offsets[number])
        if number == 0:
            first_center, first_inverse = (center, inverse)
    return (current, first_center, first_inverse)

def reference(iterate, weights, norm_scale, norm_shift):
    kernels = weights.reshape(BLOCKS, 4, 3, 3, C, C)
    gains = norm_scale.reshape(BLOCKS, 4, C)
    offsets = norm_shift.reshape(BLOCKS, 4, C)

    def relax_block(operands):
        return block_map(operands[0], operands[1], operands[2], operands[3])[0]
    relaxed = lax.map(relax_block, (iterate, kernels, gains, offsets))
    begins = jnp.concatenate([iterate[:1], relaxed[:-1]], axis=0)

    def chain_step(carried, operands):
        begin_state, kernel_set, gain_set, offset_set = operands
        fine_end, center, inverse = block_map(begin_state, kernel_set, gain_set, offset_set)

        def coarse(incoming):
            activated = activate(incoming, gain_set[0], offset_set[0], center, inverse)
            return incoming + coarse_step * convolve(activated, kernel_set[0])
        forcing = fine_end - coarse(begin_state)
        produced = coarse(carried) + forcing
        return (produced, produced)
    final_state, block_ends = lax.scan(chain_step, iterate[0], (begins, kernels, gains, offsets))
    return block_ends
```

```python
import functools

import jax
import jax.numpy as jnp
from jax import lax
from jax.experimental import pallas as pl
from jax.experimental.pallas import tpu as pltpu
from jax.sharding import Mesh
from jax.sharding import PartitionSpec as P

MESH = pl.DeviceIdType.MESH
FINE = 0.125
COARSE = 0.5
EPSILON = 1e-05
LAYERS = 4
COLUMN = 4
SAMPLES = 2
EXCHANGES = 8
EARLY = 5


def remote(src, dst, send_sem, recv_sem, device):
    return pltpu.make_async_remote_copy(
        src_ref=src,
        dst_ref=dst,
        send_sem=send_sem,
        recv_sem=recv_sem,
        device_id=device,
        device_id_type=MESH,
    )


def kernel(
    planes,
    chips,
    iterate,
    weights,
    gains,
    offsets,
    out,
    kept,
    state,
    begin,
    kernels,
    padded,
    sums,
    passed_sums,
    forcing,
    chain,
    wide,
    coarse,
    params,
    local_sem,
    sums_send,
    sums_recv,
    pass_send,
    pass_recv,
    wide_send,
    wide_recv,
    force_send,
    force_recv,
    param_send,
    param_recv,
    start_send,
    chain_send,
    chain_recv,
    out_send,
    out_recv,
):
    side, channels = iterate.shape[1], iterate.shape[3]
    rows = side * side
    z, y, x, core = (lax.axis_index(name) for name in ("z", "y", "x", "core"))
    peers = chips * 2
    me = x * 2 + core
    entries = float(peers * SAMPLES * rows)
    position = z * COLUMN + y
    up, down = lax.rem(y + 1, COLUMN), lax.rem(y + COLUMN - 1, COLUMN)
    above, below = lax.rem(z + 1, planes), lax.rem(z + planes - 1, planes)
    next_z = jnp.where(y == COLUMN - 1, above, z)

    for layer in range(LAYERS):
        pltpu.make_async_copy(weights.at[layer], kernels.at[layer], local_sem.at[layer]).start()

    barrier = pltpu.get_barrier_semaphore()
    greeted = 0
    for step in range(1, peers):
        other = lax.rem(me + step, peers)
        pl.semaphore_signal(
            barrier,
            inc=1,
            device_id={"x": other // 2, "core": lax.rem(other, 2)},
            device_id_type=MESH,
        )
        greeted += 1
    for step in range(1, COLUMN):
        for half in range(2):
            pl.semaphore_signal(
                barrier,
                inc=1,
                device_id={"y": lax.rem(y + step, COLUMN), "core": half},
                device_id_type=MESH,
            )
            greeted += 1
    for plane, row in ((above, y), (below, y), (above, up), (below, down)):
        pl.semaphore_signal(
            barrier, inc=1, device_id={"z": plane, "y": row}, device_id_type=MESH
        )
        greeted += 1

    def peer_copy(exchange, step, sender_step):
        other = lax.rem(me + step, peers)
        sender = lax.rem(me + sender_step, peers)
        return remote(
            sums.at[exchange, me],
            sums.at[exchange, me],
            sums_send.at[exchange, step],
            sums_recv.at[exchange, sender],
            {"x": other // 2, "core": lax.rem(other, 2)},
        )

    def send_sums(exchange):
        for step in range(1, peers):
            peer_copy(exchange, step, 0).start()

    def gather_sums(exchange):
        for step in range(1, peers):
            peer_copy(exchange, step, step).wait_recv()
        total = sums[exchange, 0]
        for peer in range(1, peers):
            total = total + sums[exchange, peer]
        return total

    def statistics(total):
        center = total[0:1] / entries
        inverse = lax.rsqrt(total[1:2] / entries - center * center + EPSILON)
        return center, inverse

    place = lax.broadcasted_iota(jnp.int32, (side, channels), 0)

    def activate(source, count, center, gain, offset):
        for sample in range(count):
            for row in range(side):
                value = jnp.maximum((source[sample, row] - center) * gain + offset, 0.0)
                left = jnp.where(place == 0, 0.0, pltpu.roll(value, 1, axis=0))
                right = jnp.where(place == side - 1, 0.0, pltpu.roll(value, side - 1, axis=0))
                padded[sample, row + 1, :, 0:channels] = left.astype(jnp.bfloat16)
                padded[sample, row + 1, :, channels : 2 * channels] = value.astype(jnp.bfloat16)
                padded[sample, row + 1, :, 2 * channels :] = right.astype(jnp.bfloat16)

    def convolve(sample, kernel_at):
        total = None
        for tap in range(3):
            taken = padded[sample, tap : tap + side].reshape(rows, 3 * channels)
            product = jnp.dot(taken, kernel_at(tap), preferred_element_type=jnp.float32)
            total = product if total is None else total + product
        return total.reshape(side, side, channels)

    def folded(value):
        return jnp.sum(value.reshape(rows // 8, 8, channels), axis=0)

    def store_sums(exchange, plain, square):
        sums[exchange, me] = jnp.concatenate(
            [jnp.sum(plain, axis=0, keepdims=True), jnp.sum(square, axis=0, keepdims=True)], axis=0
        )

    edge = jnp.zeros((side, 3 * channels), jnp.bfloat16)
    for sample in range(SAMPLES):
        padded[sample, 0] = edge
        padded[sample, side + 1] = edge

    plain = square = jnp.zeros((8, channels), jnp.float32)
    for sample in range(SAMPLES):
        value = iterate[sample]
        state[sample] = value
        plain, square = plain + folded(value), square + folded(value * value)
    store_sums(0, plain, square)
    pl.semaphore_wait(barrier, greeted)
    send_sums(0)

    def start_copy(sample):
        return remote(
            iterate.at[sample],
            chain.at[0],
            start_send.at[sample],
            chain_recv.at[0],
            {"y": 2 * core + sample, "core": 1},
        )

    @pl.when(position == 0)
    def _():
        for sample in range(SAMPLES):
            start_copy(sample).start()

    def wide_copy(way, tap, slot):
        target = (up, down, up, down)[way]
        return remote(
            wide.at[slot, tap],
            wide.at[slot, tap],
            wide_send.at[way, tap],
            wide_recv.at[way, tap],
            {"y": target, "core": 1},
        )

    rightward = tuple(range(9))
    leftward = tuple(range(8, -1, -1))

    for layer in range(1):
        pltpu.make_async_copy(weights.at[layer], kernels.at[layer], local_sem.at[layer]).wait()

    @pl.when(core == 1)
    def _():
        for tap in range(9):
            wide[y, tap] = kernels[
                0, tap // 3, (tap % 3) * channels : (tap % 3 + 1) * channels
            ].astype(jnp.float32)
        for count in range(EARLY):
            wide_copy(0, rightward[count], y).start()
            wide_copy(1, leftward[count], y).start()
        pltpu.make_async_copy(weights.at[0], coarse.at[y], local_sem.at[LAYERS]).start()

    def relax(layer, carry):
        center, inverse = statistics(gather_sums(layer))
        activate(state, SAMPLES, center, gains[layer] * inverse, offsets[layer])

        @pl.when(layer > 0)
        def _():
            pltpu.make_async_copy(weights.at[layer], kernels.at[layer], local_sem.at[layer]).wait()

        plain = square = jnp.zeros((8, channels), jnp.float32)
        for sample in range(SAMPLES):
            value = state[sample] + FINE * convolve(sample, lambda tap: kernels[layer, tap])
            state[sample] = value
            plain, square = plain + folded(value), square + folded(value * value)
        store_sums(layer + 1, plain, square)
        send_sums(layer + 1)
        return carry

    lax.fori_loop(0, LAYERS, relax, 0)

    following = {"z": next_z, "y": up}
    relaxed_copy = remote(state, begin, pass_send.at[0], pass_recv.at[0], following)
    relaxed_copy.start()

    @pl.when(core == 1)
    def _():
        for count in range(EARLY, 9):
            wide_copy(0, rightward[count], y).start()
            wide_copy(1, leftward[count], y).start()

    passed_sums[0] = gather_sums(LAYERS)
    totals_copy = remote(
        passed_sums.at[0], passed_sums.at[1], pass_send.at[1], pass_recv.at[1], following
    )
    totals_copy.start()
    totals_copy.wait_recv()
    relaxed_copy.wait_recv()

    @pl.when(position == 0)
    def _():
        first = sums[0, 0]
        for peer in range(1, peers):
            first = first + sums[0, peer]
        passed_sums[1] = first
        for sample in range(SAMPLES):
            begin[sample] = iterate[sample]

    center, inverse = statistics(passed_sums[1])
    gain, offset = gains[0] * inverse, offsets[0]
    params[y, 0:1] = center
    params[y, 1:2] = gain
    params[y, 2:3] = offset

    def param_copy(step, sender_step):
        return remote(
            params.at[y],
            params.at[y],
            param_send.at[step],
            param_recv.at[lax.rem(y + sender_step, COLUMN)],
            {"y": lax.rem(y + step, COLUMN), "core": 1},
        )

    @pl.when(core == 1)
    def _():
        for step in range(1, COLUMN):
            param_copy(step, 0).start()

    activate(begin, SAMPLES, center, gain, offset)
    relaxed_copy.wait_send()
    plain = square = jnp.zeros((8, channels), jnp.float32)
    for sample in range(SAMPLES):
        increment = convolve(sample, lambda tap: kernels[0, tap])
        value = begin[sample]
        kept[sample] = value + COARSE * increment
        value = value + FINE * increment
        state[sample] = value
        plain, square = plain + folded(value), square + folded(value * value)
    store_sums(LAYERS + 1, plain, square)
    send_sums(LAYERS + 1)

    @pl.when(core == 1)
    def _():
        for count in range(EARLY):
            tap = rightward[count]
            wide_copy(0, tap, down).wait_recv()
            wide_copy(2, tap, down).start()
        for count in range(9 - EARLY):
            tap = leftward[count]
            wide_copy(1, tap, up).wait_recv()
            wide_copy(3, tap, up).start()

    def refine(layer, carry):
        center, inverse = statistics(gather_sums(LAYERS + layer))
        activate(state, SAMPLES, center, gains[layer] * inverse, offsets[layer])
        plain = square = jnp.zeros((8, channels), jnp.float32)
        for sample in range(SAMPLES):
            value = state[sample] + FINE * convolve(sample, lambda tap: kernels[layer, tap])
            state[sample] = value
            plain, square = plain + folded(value), square + folded(value * value)
        store_sums(LAYERS + layer + 1, plain, square)
        send_sums(LAYERS + layer + 1)
        return carry

    lax.fori_loop(1, LAYERS - 1, refine, 0)

    def force_copy(sample):
        return remote(
            kept.at[sample],
            forcing.at[y],
            force_send.at[sample],
            force_recv.at[y],
            {"y": 2 * core + sample, "core": 1},
        )

    last = LAYERS - 1
    center, inverse = statistics(gather_sums(LAYERS + last))
    activate(state, SAMPLES, center, gains[last] * inverse, offsets[last])
    for sample in range(SAMPLES):
        value = state[sample] + FINE * convolve(sample, lambda tap: kernels[last, tap])
        value = value - kept[sample]
        kept[sample] = value
        here = (core == 1) & (y == 2 * core + sample)

        @pl.when(here)
        def _():
            forcing[y] = kept[sample]

        @pl.when(jnp.logical_not(here))
        def _():
            force_copy(sample).start()

    holder = y // 2
    slot = lax.rem(y, 2)

    def out_copy(block):
        return remote(
            chain.at[block + 1],
            out.at[slot],
            out_send.at[block],
            out_recv.at[slot],
            {"y": block, "core": holder},
        )

    hop = remote(
        chain.at[COLUMN], chain.at[0], chain_send.at[0], chain_recv.at[0], {"z": above, "core": 1}
    )

    @pl.when(core == 1)
    def _():
        for count in range(EARLY, 9):
            wide_copy(0, rightward[count], down).wait_recv()
            wide_copy(1, leftward[count], up).wait_recv()
        for count in range(9 - EARLY, EARLY):
            wide_copy(1, leftward[count], up).wait_recv()
        for count in range(EARLY):
            wide_copy(2, rightward[count], 0).wait_recv()
        for count in range(9 - EARLY):
            wide_copy(3, leftward[count], 0).wait_recv()
        for step in range(1, COLUMN):
            origin = lax.rem(y + step, COLUMN)
            for tap in range(9):
                coarse[
                    origin, tap // 3, (tap % 3) * channels : (tap % 3 + 1) * channels
                ] = wide[origin, tap].astype(jnp.bfloat16)
            param_copy(step, step).wait_recv()
        pltpu.make_async_copy(weights.at[0], coarse.at[y], local_sem.at[LAYERS]).wait()
        for block in range(COLUMN):

            @pl.when(jnp.logical_or(block != y, y < 2))
            def _():
                remote(
                    kept.at[0],
                    forcing.at[block],
                    force_send.at[0],
                    force_recv.at[block],
                    {"y": block, "core": 1},
                ).wait_recv()

        hop.wait_recv()
        for block in range(COLUMN):
            activate(
                chain.at[pl.ds(block, 1)],
                1,
                params[block, 0:1],
                params[block, 1:2],
                params[block, 2:3],
            )
            increment = convolve(0, lambda tap: coarse[block, tap])
            chain[block + 1] = chain[block] + COARSE * increment + forcing[block]
            here = (y == block) & (holder == 1)

            @pl.when(here)
            def _():
                out[slot] = chain[block + 1]

            @pl.when(jnp.logical_not(here))
            def _():
                out_copy(block).start()

        @pl.when(z < planes - 1)
        def _():
            hop.start()

    for sample in range(SAMPLES):

        @pl.when(jnp.logical_not((core == 1) & (y == 2 + sample)))
        def _():
            remote(
                chain.at[1],
                out.at[sample],
                out_send.at[0],
                out_recv.at[sample],
                {"y": y, "core": core},
            ).wait_recv()

    for exchange in range(EXCHANGES):
        for step in range(1, peers):
            peer_copy(exchange, step, 0).wait_send()
    totals_copy.wait_send()
    for sample in range(SAMPLES):

        @pl.when(position == 0)
        def _():
            start_copy(sample).wait_send()

        @pl.when(jnp.logical_not((core == 1) & (y == 2 * core + sample)))
        def _():
            force_copy(sample).wait_send()

    @pl.when(core == 1)
    def _():
        for tap in range(9):
            wide_copy(0, tap, y).wait_send()
            wide_copy(1, tap, y).wait_send()
        for count in range(EARLY):
            wide_copy(2, rightward[count], down).wait_send()
        for count in range(9 - EARLY):
            wide_copy(3, leftward[count], up).wait_send()
        for step in range(1, COLUMN):
            param_copy(step, 0).wait_send()
        for block in range(COLUMN):

            @pl.when(jnp.logical_not((y == block) & (holder == 1)))
            def _():
                out_copy(block).wait_send()

        @pl.when(z < planes - 1)
        def _():
            hop.wait_send()


def block_solve(planes, chips, iterate, weights, gains, offsets):
    _, samples, side, _, channels = iterate.shape
    state = (samples, side, side, channels)
    peers = chips * 2
    dma = pltpu.SemaphoreType.DMA
    result = pl.pallas_call(
        functools.partial(kernel, planes, chips),
        out_shape=jax.ShapeDtypeStruct(state, jnp.float32),
        in_specs=[
            pl.BlockSpec(memory_space=pltpu.VMEM),
            pl.BlockSpec(memory_space=pl.ANY),
            pl.BlockSpec(memory_space=pltpu.VMEM),
            pl.BlockSpec(memory_space=pltpu.VMEM),
        ],
        out_specs=pl.BlockSpec(memory_space=pltpu.VMEM),
        scratch_shapes=[
            pltpu.VMEM(state, jnp.float32),
            pltpu.VMEM(state, jnp.float32),
            pltpu.VMEM(state, jnp.float32),
            pltpu.VMEM((LAYERS, 3, 3 * channels, channels), jnp.bfloat16),
            pltpu.VMEM((samples, side + 2, side, 3 * channels), jnp.bfloat16),
            pltpu.VMEM((EXCHANGES, peers, 2, channels), jnp.float32),
            pltpu.VMEM((2, 2, channels), jnp.float32),
            pltpu.VMEM((COLUMN, side, side, channels), jnp.float32),
            pltpu.VMEM((COLUMN + 1, side, side, channels), jnp.float32),
            pltpu.VMEM((COLUMN, 9, channels, channels), jnp.float32),
            pltpu.VMEM((COLUMN, 3, 3 * channels, channels), jnp.bfloat16),
            pltpu.VMEM((COLUMN, 8, channels), jnp.float32),
            dma((LAYERS + 1,)),
            dma((EXCHANGES, peers)),
            dma((EXCHANGES, peers)),
            dma((2,)),
            dma((2,)),
            dma((4, 9)),
            dma((4, 9)),
            dma((samples,)),
            dma((COLUMN,)),
            dma((COLUMN,)),
            dma((COLUMN,)),
            dma((samples,)),
            dma((1,)),
            dma((1,)),
            dma((COLUMN,)),
            dma((samples,)),
        ],
        compiler_params=pltpu.CompilerParams(
            collective_id=0, has_side_effects=True, vmem_limit_bytes=60 << 20
        ),
    )(
        iterate[0],
        weights.reshape(LAYERS, 3, 3 * channels, channels),
        gains.reshape(LAYERS, 1, channels),
        offsets.reshape(LAYERS, 1, channels),
    )
    return result[None]


def solution(mesh):
    planes = mesh.shape["depth"] // COLUMN
    chips = mesh.shape["batch"] // 2
    finer = Mesh(
        mesh.devices.reshape(planes, COLUMN, chips, 2), ("z", "y", "x", "core")
    )
    depth, batch = ("z", "y"), ("x", "core")
    return jax.shard_map(
        functools.partial(block_solve, planes, chips),
        mesh=finer,
        in_specs=(
            P(depth, batch, None, None, None),
            P(depth, None, None, None, None),
            P(depth, None),
            P(depth, None),
        ),
        out_specs=P(depth, batch, None, None, None),
        check_vma=False,
    )
```

```python
import functools

import jax
import jax.numpy as jnp
from jax import lax
from jax.experimental import pallas as pl
from jax.experimental.pallas import tpu as pltpu
from jax.sharding import Mesh
from jax.sharding import PartitionSpec as P

MESH = pl.DeviceIdType.MESH
FINE = 0.125
COARSE = 0.5
EPSILON = 1e-05
LAYERS = 4
COLUMN = 4
SAMPLES = 2
EXCHANGES = 8
EARLY = 7
RELAYED = 5
HALVES = 2


def remote(src, dst, send_sem, recv_sem, device):
    return pltpu.make_async_remote_copy(
        src_ref=src,
        dst_ref=dst,
        send_sem=send_sem,
        recv_sem=recv_sem,
        device_id=device,
        device_id_type=MESH,
    )


def kernel(
    planes,
    chips,
    iterate,
    weights,
    gains,
    offsets,
    out,
    kept,
    state,
    begin,
    kernels,
    padded,
    sums,
    passed_sums,
    forcing,
    chain,
    wide,
    coarse,
    params,
    local_sem,
    sums_send,
    sums_recv,
    pass_send,
    pass_recv,
    wide_send,
    wide_recv,
    force_send,
    force_recv,
    param_send,
    param_recv,
    start_send,
    chain_send,
    chain_recv,
    out_send,
    out_recv,
):
    side, channels = iterate.shape[1], iterate.shape[3]
    rows = side * side
    z, y, x, core = (lax.axis_index(name) for name in ("z", "y", "x", "core"))
    peers = chips * 2
    me = x * 2 + core
    entries = float(peers * SAMPLES * rows)
    position = z * COLUMN + y
    up, down = lax.rem(y + 1, COLUMN), lax.rem(y + COLUMN - 1, COLUMN)
    above = lax.rem(z + 1, planes)
    next_z = jnp.where(y == COLUMN - 1, above, z)

    for layer in range(LAYERS):
        pltpu.make_async_copy(weights.at[layer], kernels.at[layer], local_sem.at[layer]).start()

    barrier = pltpu.get_barrier_semaphore()

    def greet(device):
        pl.semaphore_signal(barrier, inc=1, device_id=device, device_id_type=MESH)

    for step in range(1, peers):
        other = lax.rem(me + step, peers)
        greet({"x": other // 2, "core": lax.rem(other, 2)})
    for step in range(1, COLUMN):
        greet({"y": lax.rem(y + step, COLUMN), "core": 1})

    @pl.when(core == 1)
    def _():
        for step in range(1, COLUMN):
            greet({"y": lax.rem(y + step, COLUMN), "core": 0})

    @pl.when(position > 0)
    def _():
        greet({"z": jnp.where(y == 0, z - 1, z), "y": down})

    @pl.when((core == 1) & (z > 0))
    def _():
        greet({"z": z - 1})

    final = planes * COLUMN - 1
    greeted = (
        peers - 1
        + (COLUMN - 1) * (1 + core)
        + jnp.where(position < final, 1, 0)
        + jnp.where(z < planes - 1, core, 0)
    )

    def peer_copy(exchange, step, sender_step):
        other = lax.rem(me + step, peers)
        sender = lax.rem(me + sender_step, peers)
        return remote(
            sums.at[exchange, me],
            sums.at[exchange, me],
            sums_send.at[exchange, step],
            sums_recv.at[exchange, sender],
            {"x": other // 2, "core": lax.rem(other, 2)},
        )

    def send_sums(exchange):
        for step in range(1, peers):
            peer_copy(exchange, step, 0).start()

    def gather_sums(exchange):
        for step in range(1, peers):
            peer_copy(exchange, step, step).wait_recv()
        total = sums[exchange, 0]
        for peer in range(1, peers):
            total = total + sums[exchange, peer]
        return total

    def statistics(total):
        center = total[0:1] / entries
        inverse = lax.rsqrt(total[1:2] / entries - center * center + EPSILON)
        return center, inverse

    place = lax.broadcasted_iota(jnp.int32, (side, channels), 0)

    def activate(source, count, center, gain, offset, taken=range(side)):
        for sample in range(count):
            for row in taken:
                value = jnp.maximum((source[sample, row] - center) * gain + offset, 0.0)
                left = jnp.where(place == 0, 0.0, pltpu.roll(value, 1, axis=0))
                right = jnp.where(place == side - 1, 0.0, pltpu.roll(value, side - 1, axis=0))
                padded[sample, row + 1, :, 0:channels] = left.astype(jnp.bfloat16)
                padded[sample, row + 1, :, channels : 2 * channels] = value.astype(jnp.bfloat16)
                padded[sample, row + 1, :, 2 * channels :] = right.astype(jnp.bfloat16)

    def convolve(sample, kernel_at, first=0, count=side):
        total = None
        for tap in range(3):
            taken = padded[sample, first + tap : first + tap + count]
            taken = taken.reshape(count * side, 3 * channels)
            product = jnp.dot(taken, kernel_at(tap), preferred_element_type=jnp.float32)
            total = product if total is None else total + product
        return total.reshape(count, side, channels)

    def folded(value):
        return jnp.sum(value.reshape(rows // 8, 8, channels), axis=0)

    def store_sums(exchange, plain, square):
        sums[exchange, me] = jnp.concatenate(
            [jnp.sum(plain, axis=0, keepdims=True), jnp.sum(square, axis=0, keepdims=True)], axis=0
        )

    edge = jnp.zeros((side, 3 * channels), jnp.bfloat16)
    for sample in range(SAMPLES):
        padded[sample, 0] = edge
        padded[sample, side + 1] = edge

    plain = square = jnp.zeros((8, channels), jnp.float32)
    for sample in range(SAMPLES):
        value = iterate[sample]
        state[sample] = value
        plain, square = plain + folded(value), square + folded(value * value)
    store_sums(0, plain, square)
    pl.semaphore_wait(barrier, greeted)
    send_sums(0)

    half = side // HALVES

    def start_copy(sample, part):
        return remote(
            iterate.at[sample, pl.ds(part * half, half)],
            chain.at[0, pl.ds(part * half, half)],
            start_send.at[sample, part],
            chain_recv.at[part],
            {"y": 2 * core + sample, "core": 1},
        )

    @pl.when(position == 0)
    def _():
        for sample in range(SAMPLES):
            for part in range(HALVES):
                start_copy(sample, part).start()

    def wide_copy(way, tap, slot):
        target = (up, down, up, down)[way]
        return remote(
            wide.at[slot, tap],
            wide.at[slot, tap],
            wide_send.at[way, tap],
            wide_recv.at[way, tap],
            {"y": target, "core": 1},
        )

    rightward = tuple(range(9))
    leftward = tuple(range(8, -1, -1))

    for layer in range(1):
        pltpu.make_async_copy(weights.at[layer], kernels.at[layer], local_sem.at[layer]).wait()

    @pl.when(core == 1)
    def _():
        for tap in range(9):
            wide[y, tap] = kernels[
                0, tap // 3, (tap % 3) * channels : (tap % 3 + 1) * channels
            ].astype(jnp.float32)
        for count in range(EARLY):
            wide_copy(0, rightward[count], y).start()
            wide_copy(1, leftward[count], y).start()
        pltpu.make_async_copy(weights.at[0], coarse.at[y], local_sem.at[LAYERS]).start()

    def relax(layer, carry):
        center, inverse = statistics(gather_sums(layer))
        activate(state, SAMPLES, center, gains[pl.ds(layer, 1)] * inverse, offsets[pl.ds(layer, 1)])

        @pl.when(layer > 0)
        def _():
            pltpu.make_async_copy(weights.at[layer], kernels.at[layer], local_sem.at[layer]).wait()

        plain = square = jnp.zeros((8, channels), jnp.float32)
        for sample in range(SAMPLES):
            value = state[sample] + FINE * convolve(sample, lambda tap: kernels[layer, tap])
            state[sample] = value
            plain, square = plain + folded(value), square + folded(value * value)
        store_sums(layer + 1, plain, square)
        send_sums(layer + 1)
        return carry

    lax.fori_loop(0, LAYERS, relax, 0)

    following = {"z": next_z, "y": up}
    relaxed_copy = remote(state, begin, pass_send.at[0], pass_recv.at[0], following)

    @pl.when(position < final)
    def _():
        relaxed_copy.start()

    @pl.when(core == 1)
    def _():
        for count in range(EARLY, 9):
            wide_copy(0, rightward[count], y).start()
            wide_copy(1, leftward[count], y).start()

    passed_sums[0] = gather_sums(LAYERS)
    totals_copy = remote(
        passed_sums.at[0], passed_sums.at[1], pass_send.at[1], pass_recv.at[1], following
    )

    @pl.when(position < final)
    def _():
        totals_copy.start()

    @pl.when(position > 0)
    def _():
        totals_copy.wait_recv()
        relaxed_copy.wait_recv()

    @pl.when(position == 0)
    def _():
        first = sums[0, 0]
        for peer in range(1, peers):
            first = first + sums[0, peer]
        passed_sums[1] = first
        for sample in range(SAMPLES):
            begin[sample] = iterate[sample]

    center, inverse = statistics(passed_sums[1])
    gain, offset = gains[0:1] * inverse, offsets[0:1]
    params[y, 0:1] = center
    params[y, 1:2] = gain
    params[y, 2:3] = offset

    def param_copy(step, sender_step):
        return remote(
            params.at[y],
            params.at[y],
            param_send.at[step],
            param_recv.at[lax.rem(y + sender_step, COLUMN)],
            {"y": lax.rem(y + step, COLUMN), "core": 1},
        )

    @pl.when(core == 1)
    def _():
        for step in range(1, COLUMN):
            param_copy(step, 0).start()

    activate(begin, SAMPLES, center, gain, offset)

    @pl.when(position < final)
    def _():
        relaxed_copy.wait_send()

    plain = square = jnp.zeros((8, channels), jnp.float32)
    for sample in range(SAMPLES):
        increment = convolve(sample, lambda tap: kernels[0, tap])
        value = begin[sample]
        kept[sample] = value + COARSE * increment
        value = value + FINE * increment
        state[sample] = value
        plain, square = plain + folded(value), square + folded(value * value)
    store_sums(LAYERS + 1, plain, square)
    send_sums(LAYERS + 1)

    @pl.when(core == 1)
    def _():
        for count in range(RELAYED):
            tap = rightward[count]
            wide_copy(0, tap, down).wait_recv()
            wide_copy(2, tap, down).start()
            if count < 9 - RELAYED:
                tap = leftward[count]
                wide_copy(1, tap, up).wait_recv()
                wide_copy(3, tap, up).start()

    def refine(layer, carry):
        center, inverse = statistics(gather_sums(LAYERS + layer))
        activate(state, SAMPLES, center, gains[pl.ds(layer, 1)] * inverse, offsets[pl.ds(layer, 1)])
        plain = square = jnp.zeros((8, channels), jnp.float32)
        for sample in range(SAMPLES):
            value = state[sample] + FINE * convolve(sample, lambda tap: kernels[layer, tap])
            state[sample] = value
            plain, square = plain + folded(value), square + folded(value * value)
        store_sums(LAYERS + layer + 1, plain, square)
        send_sums(LAYERS + layer + 1)
        return carry

    lax.fori_loop(1, LAYERS - 1, refine, 0)

    def force_copy(sample):
        return remote(
            kept.at[sample],
            forcing.at[y],
            force_send.at[sample],
            force_recv.at[y],
            {"y": 2 * core + sample, "core": 1},
        )

    last = LAYERS - 1
    center, inverse = statistics(gather_sums(LAYERS + last))
    activate(state, SAMPLES, center, gains[last : last + 1] * inverse, offsets[last : last + 1])
    for sample in range(SAMPLES):
        value = state[sample] + FINE * convolve(sample, lambda tap: kernels[last, tap])
        value = value - kept[sample]
        kept[sample] = value
        here = (core == 1) & (y == 2 * core + sample)

        @pl.when(here)
        def _():
            forcing[y] = kept[sample]

        @pl.when(jnp.logical_not(here))
        def _():
            force_copy(sample).start()

    holder = y // 2
    slot = lax.rem(y, 2)

    def out_copy(block):
        return remote(
            chain.at[block + 1],
            out.at[slot],
            out_send.at[block],
            out_recv.at[slot],
            {"y": block, "core": holder},
        )

    def hop(part):
        return remote(
            chain.at[COLUMN, pl.ds(part * half, half)],
            chain.at[0, pl.ds(part * half, half)],
            chain_send.at[part],
            chain_recv.at[part],
            {"z": above, "core": 1},
        )

    def own_copy(block):
        return pltpu.make_async_copy(chain.at[block + 1], out.at[slot], local_sem.at[LAYERS + 1])

    @pl.when(core == 1)
    def _():
        for count in range(RELAYED, 9):
            wide_copy(0, rightward[count], down).wait_recv()
        for count in range(9 - RELAYED, 9):
            wide_copy(1, leftward[count], up).wait_recv()
        for count in range(RELAYED):
            wide_copy(2, rightward[count], 0).wait_recv()
        for count in range(9 - RELAYED):
            wide_copy(3, leftward[count], 0).wait_recv()
        for step in range(1, COLUMN):
            origin = lax.rem(y + step, COLUMN)
            for tap in range(9):
                coarse[
                    origin, tap // 3, (tap % 3) * channels : (tap % 3 + 1) * channels
                ] = wide[origin, tap].astype(jnp.bfloat16)
            param_copy(step, step).wait_recv()
        pltpu.make_async_copy(weights.at[0], coarse.at[y], local_sem.at[LAYERS]).wait()
        for block in range(COLUMN):
            center, gain, offset = (params[block, row : row + 1] for row in range(3))
            source = chain.at[pl.ds(block, 1)]
            if block == 0:
                for part in range(HALVES):
                    hop(part).wait_recv()
                    activate(source, 1, center, gain, offset, range(part * half, part * half + half))
            else:
                activate(source, 1, center, gain, offset)

            @pl.when(jnp.logical_or(block != y, y < 2))
            def _():
                remote(
                    kept.at[0],
                    forcing.at[block],
                    force_send.at[0],
                    force_recv.at[block],
                    {"y": block, "core": 1},
                ).wait_recv()

            if block < COLUMN - 1:
                increment = convolve(0, lambda tap: coarse[block, tap])
                chain[block + 1] = chain[block] + COARSE * increment + forcing[block]
            else:
                for part in range(HALVES):
                    first = part * half
                    taken = pl.ds(first, half)
                    increment = convolve(0, lambda tap: coarse[block, tap], first, half)
                    chain[block + 1, taken] = (
                        chain[block, taken] + COARSE * increment + forcing[block, taken]
                    )

                    @pl.when(z < planes - 1)
                    def _():
                        hop(part).start()

            here = (y == block) & (holder == 1)

            @pl.when(here)
            def _():
                own_copy(block).start()

            @pl.when(jnp.logical_not(here))
            def _():
                out_copy(block).start()

        @pl.when(holder == 1)
        def _():
            own_copy(0).wait()

    for sample in range(SAMPLES):

        @pl.when(jnp.logical_not((core == 1) & (y == 2 + sample)))
        def _():
            remote(
                chain.at[1],
                out.at[sample],
                out_send.at[0],
                out_recv.at[sample],
                {"y": y, "core": core},
            ).wait_recv()

    for exchange in range(EXCHANGES):
        for step in range(1, peers):
            peer_copy(exchange, step, 0).wait_send()

    @pl.when(position < final)
    def _():
        totals_copy.wait_send()

    for sample in range(SAMPLES):

        @pl.when(position == 0)
        def _():
            for part in range(HALVES):
                start_copy(sample, part).wait_send()

        @pl.when(jnp.logical_not((core == 1) & (y == 2 * core + sample)))
        def _():
            force_copy(sample).wait_send()

    @pl.when(core == 1)
    def _():
        for tap in range(9):
            wide_copy(0, tap, y).wait_send()
            wide_copy(1, tap, y).wait_send()
        for count in range(RELAYED):
            wide_copy(2, rightward[count], down).wait_send()
        for count in range(9 - RELAYED):
            wide_copy(3, leftward[count], up).wait_send()
        for step in range(1, COLUMN):
            param_copy(step, 0).wait_send()
        for block in range(COLUMN):

            @pl.when(jnp.logical_not((y == block) & (holder == 1)))
            def _():
                out_copy(block).wait_send()

        @pl.when(z < planes - 1)
        def _():
            for part in range(HALVES):
                hop(part).wait_send()


def block_solve(planes, chips, iterate, weights, gains, offsets):
    _, samples, side, _, channels = iterate.shape
    state = (samples, side, side, channels)
    peers = chips * 2
    dma = pltpu.SemaphoreType.DMA
    result = pl.pallas_call(
        functools.partial(kernel, planes, chips),
        out_shape=jax.ShapeDtypeStruct(state, jnp.float32),
        in_specs=[
            pl.BlockSpec(memory_space=pltpu.VMEM),
            pl.BlockSpec(memory_space=pl.ANY),
            pl.BlockSpec(memory_space=pltpu.VMEM),
            pl.BlockSpec(memory_space=pltpu.VMEM),
        ],
        out_specs=pl.BlockSpec(memory_space=pl.ANY),
        scratch_shapes=[
            pltpu.VMEM(state, jnp.float32),
            pltpu.VMEM(state, jnp.float32),
            pltpu.VMEM(state, jnp.float32),
            pltpu.VMEM((LAYERS, 3, 3 * channels, channels), jnp.bfloat16),
            pltpu.VMEM((samples, side + 2, side, 3 * channels), jnp.bfloat16),
            pltpu.VMEM((EXCHANGES, peers, 2, channels), jnp.float32),
            pltpu.VMEM((2, 2, channels), jnp.float32),
            pltpu.VMEM((COLUMN, side, side, channels), jnp.float32),
            pltpu.VMEM((COLUMN + 1, side, side, channels), jnp.float32),
            pltpu.VMEM((COLUMN, 9, channels, channels), jnp.float32),
            pltpu.VMEM((COLUMN, 3, 3 * channels, channels), jnp.bfloat16),
            pltpu.VMEM((COLUMN, 8, channels), jnp.float32),
            dma((LAYERS + 2,)),
            dma((EXCHANGES, peers)),
            dma((EXCHANGES, peers)),
            dma((2,)),
            dma((2,)),
            dma((4, 9)),
            dma((4, 9)),
            dma((samples,)),
            dma((COLUMN,)),
            dma((COLUMN,)),
            dma((COLUMN,)),
            dma((samples, HALVES)),
            dma((HALVES,)),
            dma((HALVES,)),
            dma((COLUMN,)),
            dma((samples,)),
        ],
        compiler_params=pltpu.CompilerParams(
            collective_id=0, has_side_effects=True, vmem_limit_bytes=60 << 20
        ),
    )(
        iterate[0],
        weights.reshape(LAYERS, 3, 3 * channels, channels),
        gains,
        offsets,
    )
    return result[None]


def solution(mesh):
    planes = mesh.shape["depth"] // COLUMN
    chips = mesh.shape["batch"] // 2
    finer = Mesh(
        mesh.devices.reshape(planes, COLUMN, chips, 2), ("z", "y", "x", "core")
    )
    depth, batch = ("z", "y"), ("x", "core")
    return jax.shard_map(
        functools.partial(block_solve, planes, chips),
        mesh=finer,
        in_specs=(
            P(depth, batch, None, None, None),
            P(depth, None, None, None, None),
            P(depth, None),
            P(depth, None),
        ),
        out_specs=P(depth, batch, None, None, None),
        check_vma=False,
    )
```

```python
import functools

import jax
import jax.numpy as jnp
from jax import lax
from jax.experimental import pallas as pl
from jax.experimental.pallas import tpu as pltpu
from jax.sharding import Mesh
from jax.sharding import PartitionSpec as P

MESH = pl.DeviceIdType.MESH
FINE = 0.125
COARSE = 0.5
EPSILON = 1e-05
LAYERS = 4
COLUMN = 4
SAMPLES = 2
EXCHANGES = 8
DIRECT = 5
SHARED = 4
HALVES = 2


def remote(src, dst, send_sem, recv_sem, device):
    return pltpu.make_async_remote_copy(
        src_ref=src,
        dst_ref=dst,
        send_sem=send_sem,
        recv_sem=recv_sem,
        device_id=device,
        device_id_type=MESH,
    )


def kernel(
    planes,
    chips,
    iterate,
    weights,
    gains,
    offsets,
    out,
    kept,
    state,
    begin,
    kernels,
    padded,
    sums,
    passed_sums,
    forcing,
    chain,
    wide,
    coarse,
    params,
    local_sem,
    sums_send,
    sums_recv,
    pass_send,
    pass_recv,
    wide_send,
    wide_recv,
    force_send,
    force_recv,
    param_send,
    param_recv,
    start_send,
    chain_send,
    chain_recv,
    out_send,
    out_recv,
):
    side, channels = iterate.shape[1], iterate.shape[3]
    rows = side * side
    z, y, x, core = (lax.axis_index(name) for name in ("z", "y", "x", "core"))
    peers = chips * 2
    me = x * 2 + core
    entries = float(peers * SAMPLES * rows)
    position = z * COLUMN + y
    up, down = lax.rem(y + 1, COLUMN), lax.rem(y + COLUMN - 1, COLUMN)
    above = lax.rem(z + 1, planes)
    next_z = jnp.where(y == COLUMN - 1, above, z)

    for layer in range(LAYERS):
        pltpu.make_async_copy(weights.at[layer], kernels.at[layer], local_sem.at[layer]).start()

    barrier = pltpu.get_barrier_semaphore()

    def greet(device):
        pl.semaphore_signal(barrier, inc=1, device_id=device, device_id_type=MESH)

    for step in range(1, peers):
        other = lax.rem(me + step, peers)
        greet({"x": other // 2, "core": lax.rem(other, 2)})
    for step in range(1, COLUMN):
        greet({"y": lax.rem(y + step, COLUMN), "core": 1})

    @pl.when(core == 1)
    def _():
        for step in range(1, COLUMN):
            greet({"y": lax.rem(y + step, COLUMN), "core": 0})

    @pl.when(position > 0)
    def _():
        greet({"z": jnp.where(y == 0, z - 1, z), "y": down})

    @pl.when((core == 1) & (z > 0))
    def _():
        greet({"z": z - 1})

    final = planes * COLUMN - 1
    greeted = (
        peers - 1
        + (COLUMN - 1) * (1 + core)
        + jnp.where(position < final, 1, 0)
        + jnp.where(z < planes - 1, core, 0)
    )

    def peer_copy(exchange, step, sender_step):
        other = lax.rem(me + step, peers)
        sender = lax.rem(me + sender_step, peers)
        return remote(
            sums.at[exchange, me],
            sums.at[exchange, me],
            sums_send.at[exchange, step],
            sums_recv.at[exchange, sender],
            {"x": other // 2, "core": lax.rem(other, 2)},
        )

    def send_sums(exchange):
        for step in range(1, peers):
            peer_copy(exchange, step, 0).start()

    def gather_sums(exchange):
        for step in range(1, peers):
            peer_copy(exchange, step, step).wait_recv()
        total = sums[exchange, 0]
        for peer in range(1, peers):
            total = total + sums[exchange, peer]
        return total

    def statistics(total):
        center = total[0:1] / entries
        inverse = lax.rsqrt(total[1:2] / entries - center * center + EPSILON)
        return center, inverse

    place = lax.broadcasted_iota(jnp.int32, (side, channels), 0)

    def activate(source, count, center, gain, offset, taken=range(side)):
        for sample in range(count):
            for row in taken:
                value = jnp.maximum((source[sample, row] - center) * gain + offset, 0.0)
                left = jnp.where(place == 0, 0.0, pltpu.roll(value, 1, axis=0))
                right = jnp.where(place == side - 1, 0.0, pltpu.roll(value, side - 1, axis=0))
                padded[sample, row + 1, :, 0:channels] = left.astype(jnp.bfloat16)
                padded[sample, row + 1, :, channels : 2 * channels] = value.astype(jnp.bfloat16)
                padded[sample, row + 1, :, 2 * channels :] = right.astype(jnp.bfloat16)

    def convolve(sample, kernel_at, first=0, count=side):
        total = None
        for tap in range(3):
            taken = padded[sample, first + tap : first + tap + count]
            taken = taken.reshape(count * side, 3 * channels)
            product = jnp.dot(taken, kernel_at(tap), preferred_element_type=jnp.float32)
            total = product if total is None else total + product
        return total.reshape(count, side, channels)

    def folded(value):
        return jnp.sum(value.reshape(rows // 8, 8, channels), axis=0)

    def store_sums(exchange, plain, square):
        sums[exchange, me] = jnp.concatenate(
            [jnp.sum(plain, axis=0, keepdims=True), jnp.sum(square, axis=0, keepdims=True)], axis=0
        )

    edge = jnp.zeros((side, 3 * channels), jnp.bfloat16)
    for sample in range(SAMPLES):
        padded[sample, 0] = edge
        padded[sample, side + 1] = edge

    plain = square = jnp.zeros((8, channels), jnp.float32)
    for sample in range(SAMPLES):
        value = iterate[sample]
        state[sample] = value
        plain, square = plain + folded(value), square + folded(value * value)
    store_sums(0, plain, square)
    pl.semaphore_wait(barrier, greeted)
    send_sums(0)

    half = side // HALVES

    def start_copy(sample, part):
        return remote(
            iterate.at[sample, pl.ds(part * half, half)],
            chain.at[0, pl.ds(part * half, half)],
            start_send.at[sample, part],
            chain_recv.at[part],
            {"y": 2 * core + sample, "core": 1},
        )

    @pl.when(position == 0)
    def _():
        for sample in range(SAMPLES):
            for part in range(HALVES):
                start_copy(sample, part).start()

    odd = lax.rem(x, 2) == 1

    def wide_copy(way, count, slot):
        flipped = jnp.logical_not(odd) if way % 2 else odd
        tap = jnp.where(flipped, 8 - count, count)
        if way < 4:
            device = {"y": down if way % 2 else up, "core": 1}
        else:
            device = {"x": jnp.where(odd, x - 1, x + 1), "core": 1}
        return remote(
            wide.at[slot, tap],
            wide.at[slot, tap],
            wide_send.at[way, count],
            wide_recv.at[way, count],
            device,
        )

    def pair_copy(way, count):
        return wide_copy(4 + way, count, up if way else down)

    for layer in range(1):
        pltpu.make_async_copy(weights.at[layer], kernels.at[layer], local_sem.at[layer]).wait()

    @pl.when(core == 1)
    def _():
        for tap in range(9):
            wide[y, tap] = kernels[
                0, tap // 3, (tap % 3) * channels : (tap % 3 + 1) * channels
            ].astype(jnp.float32)
        for count in range(DIRECT):
            wide_copy(0, count, y).start()
            wide_copy(1, count, y).start()
        pltpu.make_async_copy(weights.at[0], coarse.at[y], local_sem.at[LAYERS]).start()

    def relax(layer, carry):
        center, inverse = statistics(gather_sums(layer))
        activate(state, SAMPLES, center, gains[pl.ds(layer, 1)] * inverse, offsets[pl.ds(layer, 1)])

        @pl.when(layer > 0)
        def _():
            pltpu.make_async_copy(weights.at[layer], kernels.at[layer], local_sem.at[layer]).wait()

        plain = square = jnp.zeros((8, channels), jnp.float32)
        for sample in range(SAMPLES):
            value = state[sample] + FINE * convolve(sample, lambda tap: kernels[layer, tap])
            state[sample] = value
            plain, square = plain + folded(value), square + folded(value * value)
        store_sums(layer + 1, plain, square)
        send_sums(layer + 1)
        for way in range(2):

            @pl.when((core == 1) & (layer == 1 + way))
            def _():
                wide_copy(way, 0, y).wait_recv()
                pair_copy(way, 0).start()

        return carry

    lax.fori_loop(0, LAYERS, relax, 0)

    following = {"z": next_z, "y": up}
    relaxed_copy = remote(state, begin, pass_send.at[0], pass_recv.at[0], following)

    @pl.when(position < final)
    def _():
        relaxed_copy.start()

    @pl.when(core == 1)
    def _():
        for count in range(1, DIRECT):
            for way in range(2):
                wide_copy(way, count, y).wait_recv()
                if count < SHARED - 1:
                    pair_copy(way, count).start()
        for count in range(DIRECT):
            wide_copy(2, count, down).start()
            if count < 9 - DIRECT:
                wide_copy(3, count, up).start()

    passed_sums[0] = gather_sums(LAYERS)
    totals_copy = remote(
        passed_sums.at[0], passed_sums.at[1], pass_send.at[1], pass_recv.at[1], following
    )

    @pl.when(position < final)
    def _():
        totals_copy.start()

    @pl.when(position > 0)
    def _():
        totals_copy.wait_recv()
        relaxed_copy.wait_recv()

    @pl.when(position == 0)
    def _():
        first = sums[0, 0]
        for peer in range(1, peers):
            first = first + sums[0, peer]
        passed_sums[1] = first
        for sample in range(SAMPLES):
            begin[sample] = iterate[sample]

    center, inverse = statistics(passed_sums[1])
    gain, offset = gains[0:1] * inverse, offsets[0:1]
    params[y, 0:1] = center
    params[y, 1:2] = gain
    params[y, 2:3] = offset

    def param_copy(step, sender_step):
        return remote(
            params.at[y],
            params.at[y],
            param_send.at[step],
            param_recv.at[lax.rem(y + sender_step, COLUMN)],
            {"y": lax.rem(y + step, COLUMN), "core": 1},
        )

    @pl.when(core == 1)
    def _():
        for step in range(1, COLUMN):
            param_copy(step, 0).start()

    activate(begin, SAMPLES, center, gain, offset)

    @pl.when(position < final)
    def _():
        relaxed_copy.wait_send()

    plain = square = jnp.zeros((8, channels), jnp.float32)
    for sample in range(SAMPLES):
        increment = convolve(sample, lambda tap: kernels[0, tap])
        value = begin[sample]
        kept[sample] = value + COARSE * increment
        value = value + FINE * increment
        state[sample] = value
        plain, square = plain + folded(value), square + folded(value * value)
    store_sums(LAYERS + 1, plain, square)
    send_sums(LAYERS + 1)

    @pl.when(core == 1)
    def _():
        pair_copy(0, SHARED - 1).start()

    def refine(layer, carry):
        center, inverse = statistics(gather_sums(LAYERS + layer))
        activate(state, SAMPLES, center, gains[pl.ds(layer, 1)] * inverse, offsets[pl.ds(layer, 1)])
        plain = square = jnp.zeros((8, channels), jnp.float32)
        for sample in range(SAMPLES):
            value = state[sample] + FINE * convolve(sample, lambda tap: kernels[layer, tap])
            state[sample] = value
            plain, square = plain + folded(value), square + folded(value * value)
        store_sums(LAYERS + layer + 1, plain, square)
        send_sums(LAYERS + layer + 1)

        @pl.when((core == 1) & (layer == 1))
        def _():
            pair_copy(1, SHARED - 1).start()

        return carry

    lax.fori_loop(1, LAYERS - 1, refine, 0)

    def force_copy(sample):
        return remote(
            kept.at[sample],
            forcing.at[y],
            force_send.at[sample],
            force_recv.at[y],
            {"y": 2 * core + sample, "core": 1},
        )

    last = LAYERS - 1
    center, inverse = statistics(gather_sums(LAYERS + last))
    activate(state, SAMPLES, center, gains[last : last + 1] * inverse, offsets[last : last + 1])
    for sample in range(SAMPLES):
        value = state[sample] + FINE * convolve(sample, lambda tap: kernels[last, tap])
        value = value - kept[sample]
        kept[sample] = value
        here = (core == 1) & (y == 2 * core + sample)

        @pl.when(here)
        def _():
            forcing[y] = kept[sample]

        @pl.when(jnp.logical_not(here))
        def _():
            force_copy(sample).start()

    holder = y // 2
    slot = lax.rem(y, 2)

    def out_copy(block):
        return remote(
            chain.at[block + 1],
            out.at[slot],
            out_send.at[block],
            out_recv.at[slot],
            {"y": block, "core": holder},
        )

    def hop(part):
        return remote(
            chain.at[COLUMN, pl.ds(part * half, half)],
            chain.at[0, pl.ds(part * half, half)],
            chain_send.at[part],
            chain_recv.at[part],
            {"z": above, "core": 1},
        )

    def own_copy(block):
        return pltpu.make_async_copy(chain.at[block + 1], out.at[slot], local_sem.at[LAYERS + 1])

    @pl.when(core == 1)
    def _():
        for count in range(DIRECT):
            wide_copy(2, count, 0).wait_recv()
        for count in range(9 - DIRECT):
            wide_copy(3, count, 0).wait_recv()
        for count in range(SHARED):
            pair_copy(0, count).wait_recv()
            pair_copy(1, count).wait_recv()
        for step in range(1, COLUMN):
            origin = lax.rem(y + step, COLUMN)
            for tap in range(9):
                coarse[
                    origin, tap // 3, (tap % 3) * channels : (tap % 3 + 1) * channels
                ] = wide[origin, tap].astype(jnp.bfloat16)
            param_copy(step, step).wait_recv()
        pltpu.make_async_copy(weights.at[0], coarse.at[y], local_sem.at[LAYERS]).wait()
        for block in range(COLUMN):
            center, gain, offset = (params[block, row : row + 1] for row in range(3))
            source = chain.at[pl.ds(block, 1)]
            if block == 0:
                for part in range(HALVES):
                    hop(part).wait_recv()
                    activate(source, 1, center, gain, offset, range(part * half, part * half + half))
            else:
                activate(source, 1, center, gain, offset)

            @pl.when(jnp.logical_or(block != y, y < 2))
            def _():
                remote(
                    kept.at[0],
                    forcing.at[block],
                    force_send.at[0],
                    force_recv.at[block],
                    {"y": block, "core": 1},
                ).wait_recv()

            if block < COLUMN - 1:
                increment = convolve(0, lambda tap: coarse[block, tap])
                chain[block + 1] = chain[block] + COARSE * increment + forcing[block]
            else:
                for part in range(HALVES):
                    first = part * half
                    taken = pl.ds(first, half)
                    increment = convolve(0, lambda tap: coarse[block, tap], first, half)
                    chain[block + 1, taken] = (
                        chain[block, taken] + COARSE * increment + forcing[block, taken]
                    )

                    @pl.when(z < planes - 1)
                    def _():
                        hop(part).start()

            here = (y == block) & (holder == 1)

            @pl.when(here)
            def _():
                own_copy(block).start()

            @pl.when(jnp.logical_not(here))
            def _():
                out_copy(block).start()

        @pl.when(holder == 1)
        def _():
            own_copy(0).wait()

    for sample in range(SAMPLES):

        @pl.when(jnp.logical_not((core == 1) & (y == 2 + sample)))
        def _():
            remote(
                chain.at[1],
                out.at[sample],
                out_send.at[0],
                out_recv.at[sample],
                {"y": y, "core": core},
            ).wait_recv()

    for exchange in range(EXCHANGES):
        for step in range(1, peers):
            peer_copy(exchange, step, 0).wait_send()

    @pl.when(position < final)
    def _():
        totals_copy.wait_send()

    for sample in range(SAMPLES):

        @pl.when(position == 0)
        def _():
            for part in range(HALVES):
                start_copy(sample, part).wait_send()

        @pl.when(jnp.logical_not((core == 1) & (y == 2 * core + sample)))
        def _():
            force_copy(sample).wait_send()

    @pl.when(core == 1)
    def _():
        for count in range(DIRECT):
            wide_copy(0, count, y).wait_send()
            wide_copy(1, count, y).wait_send()
            wide_copy(2, count, down).wait_send()
        for count in range(9 - DIRECT):
            wide_copy(3, count, up).wait_send()
        for count in range(SHARED):
            pair_copy(0, count).wait_send()
            pair_copy(1, count).wait_send()
        for step in range(1, COLUMN):
            param_copy(step, 0).wait_send()
        for block in range(COLUMN):

            @pl.when(jnp.logical_not((y == block) & (holder == 1)))
            def _():
                out_copy(block).wait_send()

        @pl.when(z < planes - 1)
        def _():
            for part in range(HALVES):
                hop(part).wait_send()


def block_solve(planes, chips, iterate, weights, gains, offsets):
    _, samples, side, _, channels = iterate.shape
    state = (samples, side, side, channels)
    peers = chips * 2
    dma = pltpu.SemaphoreType.DMA
    result = pl.pallas_call(
        functools.partial(kernel, planes, chips),
        out_shape=jax.ShapeDtypeStruct(state, jnp.float32),
        in_specs=[
            pl.BlockSpec(memory_space=pltpu.VMEM),
            pl.BlockSpec(memory_space=pl.ANY),
            pl.BlockSpec(memory_space=pltpu.VMEM),
            pl.BlockSpec(memory_space=pltpu.VMEM),
        ],
        out_specs=pl.BlockSpec(memory_space=pl.ANY),
        scratch_shapes=[
            pltpu.VMEM(state, jnp.float32),
            pltpu.VMEM(state, jnp.float32),
            pltpu.VMEM(state, jnp.float32),
            pltpu.VMEM((LAYERS, 3, 3 * channels, channels), jnp.bfloat16),
            pltpu.VMEM((samples, side + 2, side, 3 * channels), jnp.bfloat16),
            pltpu.VMEM((EXCHANGES, peers, 2, channels), jnp.float32),
            pltpu.VMEM((2, 2, channels), jnp.float32),
            pltpu.VMEM((COLUMN, side, side, channels), jnp.float32),
            pltpu.VMEM((COLUMN + 1, side, side, channels), jnp.float32),
            pltpu.VMEM((COLUMN, 9, channels, channels), jnp.float32),
            pltpu.VMEM((COLUMN, 3, 3 * channels, channels), jnp.bfloat16),
            pltpu.VMEM((COLUMN, 8, channels), jnp.float32),
            dma((LAYERS + 2,)),
            dma((EXCHANGES, peers)),
            dma((EXCHANGES, peers)),
            dma((2,)),
            dma((2,)),
            dma((6, DIRECT)),
            dma((6, DIRECT)),
            dma((samples,)),
            dma((COLUMN,)),
            dma((COLUMN,)),
            dma((COLUMN,)),
            dma((samples, HALVES)),
            dma((HALVES,)),
            dma((HALVES,)),
            dma((COLUMN,)),
            dma((samples,)),
        ],
        compiler_params=pltpu.CompilerParams(
            collective_id=0, has_side_effects=True, vmem_limit_bytes=60 << 20
        ),
    )(
        iterate[0],
        weights.reshape(LAYERS, 3, 3 * channels, channels),
        gains,
        offsets,
    )
    return result[None]


def solution(mesh):
    planes = mesh.shape["depth"] // COLUMN
    chips = mesh.shape["batch"] // 2
    finer = Mesh(
        mesh.devices.reshape(planes, COLUMN, chips, 2), ("z", "y", "x", "core")
    )
    depth, batch = ("z", "y"), ("x", "core")
    return jax.shard_map(
        functools.partial(block_solve, planes, chips),
        mesh=finer,
        in_specs=(
            P(depth, batch, None, None, None),
            P(depth, None, None, None, None),
            P(depth, None),
            P(depth, None),
        ),
        out_specs=P(depth, batch, None, None, None),
        check_vma=False,
    )
```

```python
import functools

import jax
import jax.numpy as jnp
from jax import lax
from jax.experimental import pallas as pl
from jax.experimental.pallas import tpu as pltpu
from jax.sharding import Mesh
from jax.sharding import PartitionSpec as P

MESH = pl.DeviceIdType.MESH
FINE = 0.125
COARSE = 0.5
EPSILON = 1e-05
LAYERS = 4
COLUMN = 4
SAMPLES = 2
EXCHANGES = 8
DIRECT_RUNS = ((0, 2), (2, 5))
UP_RUN, DOWN_RUN = (0, 5), (0, 4)
PAIR_RUNS = ((0, 2), (2, 3), (3, 4))
HALVES = 1


def remote(src, dst, send_sem, recv_sem, device):
    return pltpu.make_async_remote_copy(
        src_ref=src,
        dst_ref=dst,
        send_sem=send_sem,
        recv_sem=recv_sem,
        device_id=device,
        device_id_type=MESH,
    )


def kernel(
    planes,
    chips,
    iterate,
    weights,
    gains,
    offsets,
    out,
    kept,
    state,
    begin,
    kernels,
    padded,
    sums,
    passed_sums,
    forcing,
    chain,
    wide,
    coarse,
    params,
    local_sem,
    sums_send,
    sums_recv,
    pass_send,
    pass_recv,
    wide_send,
    wide_recv,
    force_send,
    force_recv,
    param_send,
    param_recv,
    start_send,
    chain_send,
    chain_recv,
    out_send,
    out_recv,
):
    side, channels = iterate.shape[1], iterate.shape[3]
    rows = side * side
    z, y, x, core = (lax.axis_index(name) for name in ("z", "y", "x", "core"))
    peers = chips * 2
    me = x * 2 + core
    entries = float(peers * SAMPLES * rows)
    position = z * COLUMN + y
    up, down = lax.rem(y + 1, COLUMN), lax.rem(y + COLUMN - 1, COLUMN)
    above = lax.rem(z + 1, planes)
    next_z = jnp.where(y == COLUMN - 1, above, z)

    for layer in range(LAYERS):
        pltpu.make_async_copy(weights.at[layer], kernels.at[layer], local_sem.at[layer]).start()

    barrier = pltpu.get_barrier_semaphore()

    def greet(device):
        pl.semaphore_signal(barrier, inc=1, device_id=device, device_id_type=MESH)

    for step in range(1, peers):
        other = lax.rem(me + step, peers)
        greet({"x": other // 2, "core": lax.rem(other, 2)})
    for step in range(1, COLUMN):
        greet({"y": lax.rem(y + step, COLUMN), "core": 1})

    @pl.when(core == 1)
    def _():
        for step in range(1, COLUMN):
            greet({"y": lax.rem(y + step, COLUMN), "core": 0})

    @pl.when(position > 0)
    def _():
        greet({"z": jnp.where(y == 0, z - 1, z), "y": down})

    @pl.when((core == 1) & (z > 0))
    def _():
        greet({"z": z - 1})

    final = planes * COLUMN - 1
    greeted = (
        peers - 1
        + (COLUMN - 1) * (1 + core)
        + jnp.where(position < final, 1, 0)
        + jnp.where(z < planes - 1, core, 0)
    )

    def peer_copy(exchange, step, sender_step):
        other = lax.rem(me + step, peers)
        sender = lax.rem(me + sender_step, peers)
        return remote(
            sums.at[exchange, me],
            sums.at[exchange, me],
            sums_send.at[exchange, step],
            sums_recv.at[exchange, sender],
            {"x": other // 2, "core": lax.rem(other, 2)},
        )

    def send_sums(exchange):
        for step in range(1, peers):
            peer_copy(exchange, step, 0).start()

    def gather_sums(exchange):
        for step in range(1, peers):
            peer_copy(exchange, step, step).wait_recv()
        total = sums[exchange, 0]
        for peer in range(1, peers):
            total = total + sums[exchange, peer]
        return total

    def statistics(total):
        center = total[0:1] / entries
        inverse = lax.rsqrt(total[1:2] / entries - center * center + EPSILON)
        return center, inverse

    place = lax.broadcasted_iota(jnp.int32, (side, channels), 0)

    def activate(source, count, center, gain, offset, taken=range(side)):
        for sample in range(count):
            for row in taken:
                value = jnp.maximum((source[sample, row] - center) * gain + offset, 0.0)
                left = jnp.where(place == 0, 0.0, pltpu.roll(value, 1, axis=0))
                right = jnp.where(place == side - 1, 0.0, pltpu.roll(value, side - 1, axis=0))
                padded[sample, row + 1, :, 0:channels] = left.astype(jnp.bfloat16)
                padded[sample, row + 1, :, channels : 2 * channels] = value.astype(jnp.bfloat16)
                padded[sample, row + 1, :, 2 * channels :] = right.astype(jnp.bfloat16)

    def convolve(sample, kernel_at, first=0, count=side):
        total = None
        for tap in range(3):
            taken = padded[sample, first + tap : first + tap + count]
            taken = taken.reshape(count * side, 3 * channels)
            product = jnp.dot(taken, kernel_at(tap), preferred_element_type=jnp.float32)
            total = product if total is None else total + product
        return total.reshape(count, side, channels)

    def folded(value):
        return jnp.sum(value.reshape(rows // 8, 8, channels), axis=0)

    def store_sums(exchange, plain, square):
        sums[exchange, me] = jnp.concatenate(
            [jnp.sum(plain, axis=0, keepdims=True), jnp.sum(square, axis=0, keepdims=True)], axis=0
        )

    edge = jnp.zeros((side, 3 * channels), jnp.bfloat16)
    for sample in range(SAMPLES):
        padded[sample, 0] = edge
        padded[sample, side + 1] = edge

    plain = square = jnp.zeros((8, channels), jnp.float32)
    for sample in range(SAMPLES):
        value = iterate[sample]
        state[sample] = value
        plain, square = plain + folded(value), square + folded(value * value)
    store_sums(0, plain, square)
    pl.semaphore_wait(barrier, greeted)
    send_sums(0)

    half = side // HALVES

    def start_copy(sample, part):
        return remote(
            iterate.at[sample, pl.ds(part * half, half)],
            chain.at[0, pl.ds(part * half, half)],
            start_send.at[sample, part],
            chain_recv.at[part],
            {"y": 2 * core + sample, "core": 1},
        )

    @pl.when(position == 0)
    def _():
        for sample in range(SAMPLES):
            for part in range(HALVES):
                start_copy(sample, part).start()

    odd = lax.rem(x, 2) == 1

    def wide_copy(way, run, slot):
        flipped = jnp.logical_not(odd) if way % 2 else odd
        taps = pl.ds(jnp.where(flipped, 9 - run[1], run[0]), run[1] - run[0])
        if way < 4:
            device = {"y": down if way % 2 else up, "core": 1}
        else:
            device = {"x": jnp.where(odd, x - 1, x + 1), "core": 1}
        return remote(
            wide.at[slot, taps],
            wide.at[slot, taps],
            wide_send.at[way, run[0]],
            wide_recv.at[way, run[0]],
            device,
        )

    def pair_copy(way, run):
        return wide_copy(4 + way, run, up if way else down)

    for layer in range(1):
        pltpu.make_async_copy(weights.at[layer], kernels.at[layer], local_sem.at[layer]).wait()

    @pl.when(core == 1)
    def _():
        for tap in range(9):
            wide[y, tap] = kernels[
                0, tap // 3, (tap % 3) * channels : (tap % 3 + 1) * channels
            ].astype(jnp.float32)
        for run in DIRECT_RUNS:
            wide_copy(0, run, y).start()
            wide_copy(1, run, y).start()
        pltpu.make_async_copy(weights.at[0], coarse.at[y], local_sem.at[LAYERS]).start()

    def relax(layer, carry):
        center, inverse = statistics(gather_sums(layer))
        activate(state, SAMPLES, center, gains[pl.ds(layer, 1)] * inverse, offsets[pl.ds(layer, 1)])

        @pl.when(layer > 0)
        def _():
            pltpu.make_async_copy(weights.at[layer], kernels.at[layer], local_sem.at[layer]).wait()

        plain = square = jnp.zeros((8, channels), jnp.float32)
        for sample in range(SAMPLES):
            value = state[sample] + FINE * convolve(sample, lambda tap: kernels[layer, tap])
            state[sample] = value
            plain, square = plain + folded(value), square + folded(value * value)
        store_sums(layer + 1, plain, square)
        send_sums(layer + 1)
        return carry

    lax.fori_loop(0, LAYERS, relax, 0)

    following = {"z": next_z, "y": up}
    relaxed_copy = remote(state, begin, pass_send.at[0], pass_recv.at[0], following)

    @pl.when(position < final)
    def _():
        relaxed_copy.start()

    @pl.when(core == 1)
    def _():
        for run in DIRECT_RUNS:
            for way in range(2):
                wide_copy(way, run, y).wait_recv()
        wide_copy(2, UP_RUN, down).start()
        wide_copy(3, DOWN_RUN, up).start()
        for way in range(2):
            pair_copy(way, PAIR_RUNS[0]).start()

    passed_sums[0] = gather_sums(LAYERS)
    totals_copy = remote(
        passed_sums.at[0], passed_sums.at[1], pass_send.at[1], pass_recv.at[1], following
    )

    @pl.when(position < final)
    def _():
        totals_copy.start()

    @pl.when(position > 0)
    def _():
        totals_copy.wait_recv()
        relaxed_copy.wait_recv()

    @pl.when(position == 0)
    def _():
        first = sums[0, 0]
        for peer in range(1, peers):
            first = first + sums[0, peer]
        passed_sums[1] = first
        for sample in range(SAMPLES):
            begin[sample] = iterate[sample]

    center, inverse = statistics(passed_sums[1])
    gain, offset = gains[0:1] * inverse, offsets[0:1]
    params[y, 0:1] = center
    params[y, 1:2] = gain
    params[y, 2:3] = offset

    def param_copy(step, sender_step):
        return remote(
            params.at[y],
            params.at[y],
            param_send.at[step],
            param_recv.at[lax.rem(y + sender_step, COLUMN)],
            {"y": lax.rem(y + step, COLUMN), "core": 1},
        )

    @pl.when(core == 1)
    def _():
        for step in range(1, COLUMN):
            param_copy(step, 0).start()

    activate(begin, SAMPLES, center, gain, offset)

    @pl.when(position < final)
    def _():
        relaxed_copy.wait_send()

    plain = square = jnp.zeros((8, channels), jnp.float32)
    for sample in range(SAMPLES):
        increment = convolve(sample, lambda tap: kernels[0, tap])
        value = begin[sample]
        kept[sample] = value + COARSE * increment
        value = value + FINE * increment
        state[sample] = value
        plain, square = plain + folded(value), square + folded(value * value)
    store_sums(LAYERS + 1, plain, square)
    send_sums(LAYERS + 1)

    @pl.when(core == 1)
    def _():
        pair_copy(0, PAIR_RUNS[1]).start()

    def refine(layer, carry):
        center, inverse = statistics(gather_sums(LAYERS + layer))
        activate(state, SAMPLES, center, gains[pl.ds(layer, 1)] * inverse, offsets[pl.ds(layer, 1)])
        plain = square = jnp.zeros((8, channels), jnp.float32)
        for sample in range(SAMPLES):
            value = state[sample] + FINE * convolve(sample, lambda tap: kernels[layer, tap])
            state[sample] = value
            plain, square = plain + folded(value), square + folded(value * value)
        store_sums(LAYERS + layer + 1, plain, square)
        send_sums(LAYERS + layer + 1)

        @pl.when((core == 1) & (layer == 1))
        def _():
            pair_copy(1, PAIR_RUNS[1]).start()

        @pl.when((core == 1) & (layer == 2))
        def _():
            for way in range(2):
                pair_copy(way, PAIR_RUNS[2]).start()

        return carry

    lax.fori_loop(1, LAYERS - 1, refine, 0)

    def force_copy(sample):
        return remote(
            kept.at[sample],
            forcing.at[y],
            force_send.at[sample],
            force_recv.at[y],
            {"y": 2 * core + sample, "core": 1},
        )

    last = LAYERS - 1
    center, inverse = statistics(gather_sums(LAYERS + last))
    activate(state, SAMPLES, center, gains[last : last + 1] * inverse, offsets[last : last + 1])
    for sample in range(SAMPLES):
        value = state[sample] + FINE * convolve(sample, lambda tap: kernels[last, tap])
        value = value - kept[sample]
        kept[sample] = value
        here = (core == 1) & (y == 2 * core + sample)

        @pl.when(here)
        def _():
            forcing[y] = kept[sample]

        @pl.when(jnp.logical_not(here))
        def _():
            force_copy(sample).start()

    holder = y // 2
    slot = lax.rem(y, 2)

    def out_copy(block):
        return remote(
            chain.at[block + 1],
            out.at[slot],
            out_send.at[block],
            out_recv.at[slot],
            {"y": block, "core": holder},
        )

    def hop(part):
        return remote(
            chain.at[COLUMN, pl.ds(part * half, half)],
            chain.at[0, pl.ds(part * half, half)],
            chain_send.at[part],
            chain_recv.at[part],
            {"z": above, "core": 1},
        )

    def own_copy(block):
        return pltpu.make_async_copy(chain.at[block + 1], out.at[slot], local_sem.at[LAYERS + 1])

    @pl.when(core == 1)
    def _():
        wide_copy(2, UP_RUN, 0).wait_recv()
        wide_copy(3, DOWN_RUN, 0).wait_recv()
        for run in PAIR_RUNS:
            for way in range(2):
                pair_copy(way, run).wait_recv()
        for step in range(1, COLUMN):
            origin = lax.rem(y + step, COLUMN)
            for tap in range(9):
                coarse[
                    origin, tap // 3, (tap % 3) * channels : (tap % 3 + 1) * channels
                ] = wide[origin, tap].astype(jnp.bfloat16)
            param_copy(step, step).wait_recv()
        pltpu.make_async_copy(weights.at[0], coarse.at[y], local_sem.at[LAYERS]).wait()
        for block in range(COLUMN):

            @pl.when(jnp.logical_or(block != y, y < 2))
            def _():
                remote(
                    kept.at[0],
                    forcing.at[block],
                    force_send.at[0],
                    force_recv.at[block],
                    {"y": block, "core": 1},
                ).wait_recv()

        for part in range(HALVES):
            hop(part).wait_recv()
        for block in range(COLUMN):
            center, gain, offset = (params[block, row : row + 1] for row in range(3))
            activate(chain.at[pl.ds(block, 1)], 1, center, gain, offset)
            increment = convolve(0, lambda tap: coarse[block, tap])
            chain[block + 1] = chain[block] + COARSE * increment + forcing[block]

        @pl.when(z < planes - 1)
        def _():
            for part in range(HALVES):
                hop(part).start()

        for block in range(COLUMN - 1, -1, -1):
            here = (y == block) & (holder == 1)

            @pl.when(here)
            def _():
                own_copy(block).start()

            @pl.when(jnp.logical_not(here))
            def _():
                out_copy(block).start()

        @pl.when(holder == 1)
        def _():
            own_copy(0).wait()

    for sample in range(SAMPLES):

        @pl.when(jnp.logical_not((core == 1) & (y == 2 + sample)))
        def _():
            remote(
                chain.at[1],
                out.at[sample],
                out_send.at[0],
                out_recv.at[sample],
                {"y": y, "core": core},
            ).wait_recv()

    for exchange in range(EXCHANGES):
        for step in range(1, peers):
            peer_copy(exchange, step, 0).wait_send()

    @pl.when(position < final)
    def _():
        totals_copy.wait_send()

    for sample in range(SAMPLES):

        @pl.when(position == 0)
        def _():
            for part in range(HALVES):
                start_copy(sample, part).wait_send()

        @pl.when(jnp.logical_not((core == 1) & (y == 2 * core + sample)))
        def _():
            force_copy(sample).wait_send()

    @pl.when(core == 1)
    def _():
        for run in DIRECT_RUNS:
            for way in range(2):
                wide_copy(way, run, y).wait_send()
        wide_copy(2, UP_RUN, down).wait_send()
        wide_copy(3, DOWN_RUN, up).wait_send()
        for run in PAIR_RUNS:
            for way in range(2):
                pair_copy(way, run).wait_send()
        for step in range(1, COLUMN):
            param_copy(step, 0).wait_send()
        for block in range(COLUMN):

            @pl.when(jnp.logical_not((y == block) & (holder == 1)))
            def _():
                out_copy(block).wait_send()

        @pl.when(z < planes - 1)
        def _():
            for part in range(HALVES):
                hop(part).wait_send()


def block_solve(planes, chips, iterate, weights, gains, offsets):
    _, samples, side, _, channels = iterate.shape
    state = (samples, side, side, channels)
    peers = chips * 2
    dma = pltpu.SemaphoreType.DMA
    result = pl.pallas_call(
        functools.partial(kernel, planes, chips),
        out_shape=jax.ShapeDtypeStruct(state, jnp.float32),
        in_specs=[
            pl.BlockSpec(memory_space=pltpu.VMEM),
            pl.BlockSpec(memory_space=pl.ANY),
            pl.BlockSpec(memory_space=pltpu.VMEM),
            pl.BlockSpec(memory_space=pltpu.VMEM),
        ],
        out_specs=pl.BlockSpec(memory_space=pl.ANY),
        scratch_shapes=[
            pltpu.VMEM(state, jnp.float32),
            pltpu.VMEM(state, jnp.float32),
            pltpu.VMEM(state, jnp.float32),
            pltpu.VMEM((LAYERS, 3, 3 * channels, channels), jnp.bfloat16),
            pltpu.VMEM((samples, side + 2, side, 3 * channels), jnp.bfloat16),
            pltpu.VMEM((EXCHANGES, peers, 2, channels), jnp.float32),
            pltpu.VMEM((2, 2, channels), jnp.float32),
            pltpu.VMEM((COLUMN, side, side, channels), jnp.float32),
            pltpu.VMEM((COLUMN + 1, side, side, channels), jnp.float32),
            pltpu.VMEM((COLUMN, 9, channels, channels), jnp.float32),
            pltpu.VMEM((COLUMN, 3, 3 * channels, channels), jnp.bfloat16),
            pltpu.VMEM((COLUMN, 8, channels), jnp.float32),
            dma((LAYERS + 2,)),
            dma((EXCHANGES, peers)),
            dma((EXCHANGES, peers)),
            dma((2,)),
            dma((2,)),
            dma((6, 4)),
            dma((6, 4)),
            dma((samples,)),
            dma((COLUMN,)),
            dma((COLUMN,)),
            dma((COLUMN,)),
            dma((samples, HALVES)),
            dma((HALVES,)),
            dma((HALVES,)),
            dma((COLUMN,)),
            dma((samples,)),
        ],
        compiler_params=pltpu.CompilerParams(
            collective_id=0, has_side_effects=True, vmem_limit_bytes=60 << 20
        ),
    )(
        iterate[0],
        weights.reshape(LAYERS, 3, 3 * channels, channels),
        gains,
        offsets,
    )
    return result[None]


def solution(mesh):
    planes = mesh.shape["depth"] // COLUMN
    chips = mesh.shape["batch"] // 2
    finer = Mesh(
        mesh.devices.reshape(planes, COLUMN, chips, 2), ("z", "y", "x", "core")
    )
    depth, batch = ("z", "y"), ("x", "core")
    return jax.shard_map(
        functools.partial(block_solve, planes, chips),
        mesh=finer,
        in_specs=(
            P(depth, batch, None, None, None),
            P(depth, None, None, None, None),
            P(depth, None),
            P(depth, None),
        ),
        out_specs=P(depth, batch, None, None, None),
        check_vma=False,
    )
```

```python
import functools

import jax
import jax.numpy as jnp
from jax import lax
from jax.experimental import pallas as pl
from jax.experimental.pallas import tpu as pltpu
from jax.sharding import Mesh
from jax.sharding import PartitionSpec as P

MESH = pl.DeviceIdType.MESH
FINE = 0.125
COARSE = 0.5
EPSILON = 1e-05
LAYERS = 4
COLUMN = 4
SAMPLES = 2
EXCHANGES = 8
EARLY = 7
RELAYED = 5
HALVES = 1


def remote(src, dst, send_sem, recv_sem, device):
    return pltpu.make_async_remote_copy(
        src_ref=src,
        dst_ref=dst,
        send_sem=send_sem,
        recv_sem=recv_sem,
        device_id=device,
        device_id_type=MESH,
    )


def kernel(
    planes,
    chips,
    iterate,
    weights,
    gains,
    offsets,
    out,
    kept,
    state,
    begin,
    kernels,
    padded,
    sums,
    passed_sums,
    forcing,
    chain,
    wide,
    coarse,
    params,
    local_sem,
    sums_send,
    sums_recv,
    pass_send,
    pass_recv,
    wide_send,
    wide_recv,
    force_send,
    force_recv,
    param_send,
    param_recv,
    start_send,
    chain_send,
    chain_recv,
    out_send,
    out_recv,
):
    side, channels = iterate.shape[1], iterate.shape[3]
    rows = side * side
    z, y, x, core = (lax.axis_index(name) for name in ("z", "y", "x", "core"))
    peers = chips * 2
    me = x * 2 + core
    entries = float(peers * SAMPLES * rows)
    position = z * COLUMN + y
    up, down = lax.rem(y + 1, COLUMN), lax.rem(y + COLUMN - 1, COLUMN)
    above = lax.rem(z + 1, planes)
    next_z = jnp.where(y == COLUMN - 1, above, z)

    for layer in range(LAYERS):
        pltpu.make_async_copy(weights.at[layer], kernels.at[layer], local_sem.at[layer]).start()

    barrier = pltpu.get_barrier_semaphore()

    def greet(device):
        pl.semaphore_signal(barrier, inc=1, device_id=device, device_id_type=MESH)

    for step in range(1, peers):
        other = lax.rem(me + step, peers)
        greet({"x": other // 2, "core": lax.rem(other, 2)})
    for step in range(1, COLUMN):
        greet({"y": lax.rem(y + step, COLUMN), "core": 1})

    @pl.when(core == 1)
    def _():
        for step in range(1, COLUMN):
            greet({"y": lax.rem(y + step, COLUMN), "core": 0})

    @pl.when(position > 0)
    def _():
        greet({"z": jnp.where(y == 0, z - 1, z), "y": down})

    @pl.when((core == 1) & (z > 0))
    def _():
        greet({"z": z - 1})

    final = planes * COLUMN - 1
    greeted = (
        peers - 1
        + (COLUMN - 1) * (1 + core)
        + jnp.where(position < final, 1, 0)
        + jnp.where(z < planes - 1, core, 0)
    )

    def peer_copy(exchange, step, sender_step):
        other = lax.rem(me + step, peers)
        sender = lax.rem(me + sender_step, peers)
        return remote(
            sums.at[exchange, me],
            sums.at[exchange, me],
            sums_send.at[exchange, step],
            sums_recv.at[exchange, sender],
            {"x": other // 2, "core": lax.rem(other, 2)},
        )

    def send_sums(exchange):
        for step in range(1, peers):
            peer_copy(exchange, step, 0).start()

    def gather_sums(exchange):
        for step in range(1, peers):
            peer_copy(exchange, step, step).wait_recv()
        total = sums[exchange, 0]
        for peer in range(1, peers):
            total = total + sums[exchange, peer]
        return total

    def statistics(total):
        center = total[0:1] / entries
        inverse = lax.rsqrt(total[1:2] / entries - center * center + EPSILON)
        return center, inverse

    place = lax.broadcasted_iota(jnp.int32, (side, channels), 0)

    def activate(source, count, center, gain, offset, taken=range(side)):
        for sample in range(count):
            for row in taken:
                value = jnp.maximum((source[sample, row] - center) * gain + offset, 0.0)
                left = jnp.where(place == 0, 0.0, pltpu.roll(value, 1, axis=0))
                right = jnp.where(place == side - 1, 0.0, pltpu.roll(value, side - 1, axis=0))
                padded[sample, row + 1, :, 0:channels] = left.astype(jnp.bfloat16)
                padded[sample, row + 1, :, channels : 2 * channels] = value.astype(jnp.bfloat16)
                padded[sample, row + 1, :, 2 * channels :] = right.astype(jnp.bfloat16)

    def convolve(sample, kernel_at, first=0, count=side):
        total = None
        for tap in range(3):
            taken = padded[sample, first + tap : first + tap + count]
            taken = taken.reshape(count * side, 3 * channels)
            product = jnp.dot(taken, kernel_at(tap), preferred_element_type=jnp.float32)
            total = product if total is None else total + product
        return total.reshape(count, side, channels)

    def folded(value):
        return jnp.sum(value.reshape(rows // 8, 8, channels), axis=0)

    def store_sums(exchange, plain, square):
        sums[exchange, me] = jnp.concatenate(
            [jnp.sum(plain, axis=0, keepdims=True), jnp.sum(square, axis=0, keepdims=True)], axis=0
        )

    edge = jnp.zeros((side, 3 * channels), jnp.bfloat16)
    for sample in range(SAMPLES):
        padded[sample, 0] = edge
        padded[sample, side + 1] = edge

    plain = square = jnp.zeros((8, channels), jnp.float32)
    for sample in range(SAMPLES):
        value = iterate[sample]
        state[sample] = value
        plain, square = plain + folded(value), square + folded(value * value)
    store_sums(0, plain, square)
    pl.semaphore_wait(barrier, greeted)
    send_sums(0)

    half = side // HALVES

    def start_copy(sample, part):
        return remote(
            iterate.at[sample, pl.ds(part * half, half)],
            chain.at[0, pl.ds(part * half, half)],
            start_send.at[sample, part],
            chain_recv.at[part],
            {"y": 2 * core + sample, "core": 1},
        )

    @pl.when(position == 0)
    def _():
        for sample in range(SAMPLES):
            for part in range(HALVES):
                start_copy(sample, part).start()

    def wide_copy(way, tap, slot):
        target = (up, down, up, down)[way]
        return remote(
            wide.at[slot, tap],
            wide.at[slot, tap],
            wide_send.at[way, tap],
            wide_recv.at[way, tap],
            {"y": target, "core": 1},
        )

    rightward = tuple(range(9))
    leftward = tuple(range(8, -1, -1))

    for layer in range(1):
        pltpu.make_async_copy(weights.at[layer], kernels.at[layer], local_sem.at[layer]).wait()

    @pl.when(core == 1)
    def _():
        for tap in range(9):
            wide[y, tap] = kernels[
                0, tap // 3, (tap % 3) * channels : (tap % 3 + 1) * channels
            ].astype(jnp.float32)
        for count in range(EARLY):
            wide_copy(0, rightward[count], y).start()
            wide_copy(1, leftward[count], y).start()
        pltpu.make_async_copy(weights.at[0], coarse.at[y], local_sem.at[LAYERS]).start()

    def relax(layer, carry):
        center, inverse = statistics(gather_sums(layer))
        activate(state, SAMPLES, center, gains[pl.ds(layer, 1)] * inverse, offsets[pl.ds(layer, 1)])

        @pl.when(layer > 0)
        def _():
            pltpu.make_async_copy(weights.at[layer], kernels.at[layer], local_sem.at[layer]).wait()

        plain = square = jnp.zeros((8, channels), jnp.float32)
        for sample in range(SAMPLES):
            value = state[sample] + FINE * convolve(sample, lambda tap: kernels[layer, tap])
            state[sample] = value
            plain, square = plain + folded(value), square + folded(value * value)
        store_sums(layer + 1, plain, square)
        send_sums(layer + 1)
        return carry

    lax.fori_loop(0, LAYERS, relax, 0)

    following = {"z": next_z, "y": up}
    relaxed_copy = remote(state, begin, pass_send.at[0], pass_recv.at[0], following)

    @pl.when(position < final)
    def _():
        relaxed_copy.start()

    @pl.when(core == 1)
    def _():
        for count in range(EARLY, 9):
            wide_copy(0, rightward[count], y).start()
            wide_copy(1, leftward[count], y).start()

    passed_sums[0] = gather_sums(LAYERS)
    totals_copy = remote(
        passed_sums.at[0], passed_sums.at[1], pass_send.at[1], pass_recv.at[1], following
    )

    @pl.when(position < final)
    def _():
        totals_copy.start()

    @pl.when(position > 0)
    def _():
        totals_copy.wait_recv()
        relaxed_copy.wait_recv()

    @pl.when(position == 0)
    def _():
        first = sums[0, 0]
        for peer in range(1, peers):
            first = first + sums[0, peer]
        passed_sums[1] = first
        for sample in range(SAMPLES):
            begin[sample] = iterate[sample]

    center, inverse = statistics(passed_sums[1])
    gain, offset = gains[0:1] * inverse, offsets[0:1]
    params[y, 0:1] = center
    params[y, 1:2] = gain
    params[y, 2:3] = offset

    def param_copy(step, sender_step):
        return remote(
            params.at[y],
            params.at[y],
            param_send.at[step],
            param_recv.at[lax.rem(y + sender_step, COLUMN)],
            {"y": lax.rem(y + step, COLUMN), "core": 1},
        )

    @pl.when(core == 1)
    def _():
        for step in range(1, COLUMN):
            param_copy(step, 0).start()

    activate(begin, SAMPLES, center, gain, offset)

    @pl.when(position < final)
    def _():
        relaxed_copy.wait_send()

    plain = square = jnp.zeros((8, channels), jnp.float32)
    for sample in range(SAMPLES):
        increment = convolve(sample, lambda tap: kernels[0, tap])
        value = begin[sample]
        kept[sample] = value + COARSE * increment
        value = value + FINE * increment
        state[sample] = value
        plain, square = plain + folded(value), square + folded(value * value)
    store_sums(LAYERS + 1, plain, square)
    send_sums(LAYERS + 1)

    @pl.when(core == 1)
    def _():
        for count in range(RELAYED):
            tap = rightward[count]
            wide_copy(0, tap, down).wait_recv()
            wide_copy(2, tap, down).start()
            if count < 9 - RELAYED:
                tap = leftward[count]
                wide_copy(1, tap, up).wait_recv()
                wide_copy(3, tap, up).start()

    def refine(layer, carry):
        center, inverse = statistics(gather_sums(LAYERS + layer))
        activate(state, SAMPLES, center, gains[pl.ds(layer, 1)] * inverse, offsets[pl.ds(layer, 1)])
        plain = square = jnp.zeros((8, channels), jnp.float32)
        for sample in range(SAMPLES):
            value = state[sample] + FINE * convolve(sample, lambda tap: kernels[layer, tap])
            state[sample] = value
            plain, square = plain + folded(value), square + folded(value * value)
        store_sums(LAYERS + layer + 1, plain, square)
        send_sums(LAYERS + layer + 1)
        return carry

    lax.fori_loop(1, LAYERS - 1, refine, 0)

    def force_copy(sample):
        return remote(
            kept.at[sample],
            forcing.at[y],
            force_send.at[sample],
            force_recv.at[y],
            {"y": 2 * core + sample, "core": 1},
        )

    last = LAYERS - 1
    center, inverse = statistics(gather_sums(LAYERS + last))
    activate(state, SAMPLES, center, gains[last : last + 1] * inverse, offsets[last : last + 1])
    for sample in range(SAMPLES):
        value = state[sample] + FINE * convolve(sample, lambda tap: kernels[last, tap])
        value = value - kept[sample]
        kept[sample] = value
        here = (core == 1) & (y == 2 * core + sample)

        @pl.when(here)
        def _():
            forcing[y] = kept[sample]

        @pl.when(jnp.logical_not(here))
        def _():
            force_copy(sample).start()

    holder = y // 2
    slot = lax.rem(y, 2)

    def out_copy(block):
        return remote(
            chain.at[block + 1],
            out.at[slot],
            out_send.at[block],
            out_recv.at[slot],
            {"y": block, "core": holder},
        )

    def hop(part):
        return remote(
            chain.at[COLUMN, pl.ds(part * half, half)],
            chain.at[0, pl.ds(part * half, half)],
            chain_send.at[part],
            chain_recv.at[part],
            {"z": above, "core": 1},
        )

    def own_copy(block):
        return pltpu.make_async_copy(chain.at[block + 1], out.at[slot], local_sem.at[LAYERS + 1])

    @pl.when(core == 1)
    def _():
        for count in range(RELAYED, 9):
            wide_copy(0, rightward[count], down).wait_recv()
        for count in range(9 - RELAYED, 9):
            wide_copy(1, leftward[count], up).wait_recv()
        for count in range(RELAYED):
            wide_copy(2, rightward[count], 0).wait_recv()
        for count in range(9 - RELAYED):
            wide_copy(3, leftward[count], 0).wait_recv()
        for step in range(1, COLUMN):
            origin = lax.rem(y + step, COLUMN)
            for tap in range(9):
                coarse[
                    origin, tap // 3, (tap % 3) * channels : (tap % 3 + 1) * channels
                ] = wide[origin, tap].astype(jnp.bfloat16)
            param_copy(step, step).wait_recv()
        pltpu.make_async_copy(weights.at[0], coarse.at[y], local_sem.at[LAYERS]).wait()
        for block in range(COLUMN):

            @pl.when(jnp.logical_or(block != y, y < 2))
            def _():
                remote(
                    kept.at[0],
                    forcing.at[block],
                    force_send.at[0],
                    force_recv.at[block],
                    {"y": block, "core": 1},
                ).wait_recv()

        for part in range(HALVES):
            hop(part).wait_recv()
        for block in range(COLUMN):
            center, gain, offset = (params[block, row : row + 1] for row in range(3))
            activate(chain.at[pl.ds(block, 1)], 1, center, gain, offset)
            increment = convolve(0, lambda tap: coarse[block, tap])
            chain[block + 1] = chain[block] + COARSE * increment + forcing[block]

        @pl.when(z < planes - 1)
        def _():
            for part in range(HALVES):
                hop(part).start()

        for block in range(COLUMN - 1, -1, -1):
            here = (y == block) & (holder == 1)

            @pl.when(here)
            def _():
                own_copy(block).start()

            @pl.when(jnp.logical_not(here))
            def _():
                out_copy(block).start()

        @pl.when(holder == 1)
        def _():
            own_copy(0).wait()

    for sample in range(SAMPLES):

        @pl.when(jnp.logical_not((core == 1) & (y == 2 + sample)))
        def _():
            remote(
                chain.at[1],
                out.at[sample],
                out_send.at[0],
                out_recv.at[sample],
                {"y": y, "core": core},
            ).wait_recv()

    for exchange in range(EXCHANGES):
        for step in range(1, peers):
            peer_copy(exchange, step, 0).wait_send()

    @pl.when(position < final)
    def _():
        totals_copy.wait_send()

    for sample in range(SAMPLES):

        @pl.when(position == 0)
        def _():
            for part in range(HALVES):
                start_copy(sample, part).wait_send()

        @pl.when(jnp.logical_not((core == 1) & (y == 2 * core + sample)))
        def _():
            force_copy(sample).wait_send()

    @pl.when(core == 1)
    def _():
        for tap in range(9):
            wide_copy(0, tap, y).wait_send()
            wide_copy(1, tap, y).wait_send()
        for count in range(RELAYED):
            wide_copy(2, rightward[count], down).wait_send()
        for count in range(9 - RELAYED):
            wide_copy(3, leftward[count], up).wait_send()
        for step in range(1, COLUMN):
            param_copy(step, 0).wait_send()
        for block in range(COLUMN):

            @pl.when(jnp.logical_not((y == block) & (holder == 1)))
            def _():
                out_copy(block).wait_send()

        @pl.when(z < planes - 1)
        def _():
            for part in range(HALVES):
                hop(part).wait_send()


def block_solve(planes, chips, iterate, weights, gains, offsets):
    _, samples, side, _, channels = iterate.shape
    state = (samples, side, side, channels)
    peers = chips * 2
    dma = pltpu.SemaphoreType.DMA
    result = pl.pallas_call(
        functools.partial(kernel, planes, chips),
        out_shape=jax.ShapeDtypeStruct(state, jnp.float32),
        in_specs=[
            pl.BlockSpec(memory_space=pltpu.VMEM),
            pl.BlockSpec(memory_space=pl.ANY),
            pl.BlockSpec(memory_space=pltpu.VMEM),
            pl.BlockSpec(memory_space=pltpu.VMEM),
        ],
        out_specs=pl.BlockSpec(memory_space=pl.ANY),
        scratch_shapes=[
            pltpu.VMEM(state, jnp.float32),
            pltpu.VMEM(state, jnp.float32),
            pltpu.VMEM(state, jnp.float32),
            pltpu.VMEM((LAYERS, 3, 3 * channels, channels), jnp.bfloat16),
            pltpu.VMEM((samples, side + 2, side, 3 * channels), jnp.bfloat16),
            pltpu.VMEM((EXCHANGES, peers, 2, channels), jnp.float32),
            pltpu.VMEM((2, 2, channels), jnp.float32),
            pltpu.VMEM((COLUMN, side, side, channels), jnp.float32),
            pltpu.VMEM((COLUMN + 1, side, side, channels), jnp.float32),
            pltpu.VMEM((COLUMN, 9, channels, channels), jnp.float32),
            pltpu.VMEM((COLUMN, 3, 3 * channels, channels), jnp.bfloat16),
            pltpu.VMEM((COLUMN, 8, channels), jnp.float32),
            dma((LAYERS + 2,)),
            dma((EXCHANGES, peers)),
            dma((EXCHANGES, peers)),
            dma((2,)),
            dma((2,)),
            dma((4, 9)),
            dma((4, 9)),
            dma((samples,)),
            dma((COLUMN,)),
            dma((COLUMN,)),
            dma((COLUMN,)),
            dma((samples, HALVES)),
            dma((HALVES,)),
            dma((HALVES,)),
            dma((COLUMN,)),
            dma((samples,)),
        ],
        compiler_params=pltpu.CompilerParams(
            collective_id=0, has_side_effects=True, vmem_limit_bytes=60 << 20
        ),
    )(
        iterate[0],
        weights.reshape(LAYERS, 3, 3 * channels, channels),
        gains,
        offsets,
    )
    return result[None]


def solution(mesh):
    planes = mesh.shape["depth"] // COLUMN
    chips = mesh.shape["batch"] // 2
    finer = Mesh(
        mesh.devices.reshape(planes, COLUMN, chips, 2), ("z", "y", "x", "core")
    )
    depth, batch = ("z", "y"), ("x", "core")
    return jax.shard_map(
        functools.partial(block_solve, planes, chips),
        mesh=finer,
        in_specs=(
            P(depth, batch, None, None, None),
            P(depth, None, None, None, None),
            P(depth, None),
            P(depth, None),
        ),
        out_specs=P(depth, batch, None, None, None),
        check_vma=False,
    )
```

```python
import functools

import jax
import jax.numpy as jnp
from jax import lax
from jax.experimental import pallas as pl
from jax.experimental.pallas import tpu as pltpu
from jax.sharding import Mesh
from jax.sharding import PartitionSpec as P

MESH = pl.DeviceIdType.MESH
FINE = 0.125
COARSE = 0.5
EPSILON = 1e-05
LAYERS = 4
COLUMN = 4
SAMPLES = 2
EXCHANGES = 8
DIRECT = 5
SHARED = 4
HALVES = 2


def remote(src, dst, send_sem, recv_sem, device):
    return pltpu.make_async_remote_copy(
        src_ref=src,
        dst_ref=dst,
        send_sem=send_sem,
        recv_sem=recv_sem,
        device_id=device,
        device_id_type=MESH,
    )


def kernel(
    planes,
    chips,
    iterate,
    weights,
    gains,
    offsets,
    out,
    kept,
    state,
    begin,
    kernels,
    padded,
    sums,
    passed_sums,
    forcing,
    chain,
    wide,
    coarse,
    params,
    local_sem,
    sums_send,
    sums_recv,
    pass_send,
    pass_recv,
    wide_send,
    wide_recv,
    force_send,
    force_recv,
    param_send,
    param_recv,
    start_send,
    chain_send,
    chain_recv,
    out_send,
    out_recv,
):
    side, channels = iterate.shape[1], iterate.shape[3]
    rows = side * side
    z, y, x, core = (lax.axis_index(name) for name in ("z", "y", "x", "core"))
    peers = chips * 2
    me = x * 2 + core
    entries = float(peers * SAMPLES * rows)
    position = z * COLUMN + y
    up, down = lax.rem(y + 1, COLUMN), lax.rem(y + COLUMN - 1, COLUMN)
    above = lax.rem(z + 1, planes)
    next_z = jnp.where(y == COLUMN - 1, above, z)

    for layer in range(LAYERS):
        pltpu.make_async_copy(weights.at[layer], kernels.at[layer], local_sem.at[layer]).start()

    barrier = pltpu.get_barrier_semaphore()

    def greet(device):
        pl.semaphore_signal(barrier, inc=1, device_id=device, device_id_type=MESH)

    for step in range(1, peers):
        other = lax.rem(me + step, peers)
        greet({"x": other // 2, "core": lax.rem(other, 2)})
    for step in range(1, COLUMN):
        greet({"y": lax.rem(y + step, COLUMN), "core": 1})

    @pl.when(core == 1)
    def _():
        for step in range(1, COLUMN):
            greet({"y": lax.rem(y + step, COLUMN), "core": 0})

    @pl.when(position > 0)
    def _():
        greet({"z": jnp.where(y == 0, z - 1, z), "y": down})

    @pl.when((core == 1) & (z > 0))
    def _():
        greet({"z": z - 1})

    final = planes * COLUMN - 1
    greeted = (
        peers - 1
        + (COLUMN - 1) * (1 + core)
        + jnp.where(position < final, 1, 0)
        + jnp.where(z < planes - 1, core, 0)
    )

    def peer_copy(exchange, step, sender_step):
        other = lax.rem(me + step, peers)
        sender = lax.rem(me + sender_step, peers)
        return remote(
            sums.at[exchange, me],
            sums.at[exchange, me],
            sums_send.at[exchange, step],
            sums_recv.at[exchange, sender],
            {"x": other // 2, "core": lax.rem(other, 2)},
        )

    def send_sums(exchange):
        for step in range(1, peers):
            peer_copy(exchange, step, 0).start()

    def gather_sums(exchange):
        for step in range(1, peers):
            peer_copy(exchange, step, step).wait_recv()
        total = sums[exchange, 0]
        for peer in range(1, peers):
            total = total + sums[exchange, peer]
        return total

    def statistics(total):
        center = total[0:1] / entries
        inverse = lax.rsqrt(total[1:2] / entries - center * center + EPSILON)
        return center, inverse

    place = lax.broadcasted_iota(jnp.int32, (side, channels), 0)

    def activate(source, count, center, gain, offset, taken=range(side)):
        for sample in range(count):
            for row in taken:
                value = jnp.maximum((source[sample, row] - center) * gain + offset, 0.0)
                left = jnp.where(place == 0, 0.0, pltpu.roll(value, 1, axis=0))
                right = jnp.where(place == side - 1, 0.0, pltpu.roll(value, side - 1, axis=0))
                padded[sample, row + 1, :, 0:channels] = left.astype(jnp.bfloat16)
                padded[sample, row + 1, :, channels : 2 * channels] = value.astype(jnp.bfloat16)
                padded[sample, row + 1, :, 2 * channels :] = right.astype(jnp.bfloat16)

    def convolve(sample, kernel_at, first=0, count=side):
        total = None
        for tap in range(3):
            taken = padded[sample, first + tap : first + tap + count]
            taken = taken.reshape(count * side, 3 * channels)
            product = jnp.dot(taken, kernel_at(tap), preferred_element_type=jnp.float32)
            total = product if total is None else total + product
        return total.reshape(count, side, channels)

    def folded(value):
        return jnp.sum(value.reshape(rows // 8, 8, channels), axis=0)

    def store_sums(exchange, plain, square):
        sums[exchange, me] = jnp.concatenate(
            [jnp.sum(plain, axis=0, keepdims=True), jnp.sum(square, axis=0, keepdims=True)], axis=0
        )

    edge = jnp.zeros((side, 3 * channels), jnp.bfloat16)
    for sample in range(SAMPLES):
        padded[sample, 0] = edge
        padded[sample, side + 1] = edge

    plain = square = jnp.zeros((8, channels), jnp.float32)
    for sample in range(SAMPLES):
        value = iterate[sample]
        state[sample] = value
        plain, square = plain + folded(value), square + folded(value * value)
    store_sums(0, plain, square)
    pl.semaphore_wait(barrier, greeted)
    send_sums(0)

    half = side // HALVES

    def start_copy(sample, part):
        return remote(
            iterate.at[sample, pl.ds(part * half, half)],
            chain.at[0, pl.ds(part * half, half)],
            start_send.at[sample, part],
            chain_recv.at[part],
            {"y": 2 * core + sample, "core": 1},
        )

    @pl.when(position == 0)
    def _():
        for sample in range(SAMPLES):
            for part in range(HALVES):
                start_copy(sample, part).start()

    odd = lax.rem(x, 2) == 1

    def wide_copy(way, count, slot):
        flipped = jnp.logical_not(odd) if way % 2 else odd
        tap = jnp.where(flipped, 8 - count, count)
        if way < 4:
            device = {"y": down if way % 2 else up, "core": 1}
        else:
            device = {"x": jnp.where(odd, x - 1, x + 1), "core": 1}
        return remote(
            wide.at[slot, tap],
            wide.at[slot, tap],
            wide_send.at[way, count],
            wide_recv.at[way, count],
            device,
        )

    def pair_copy(way, count):
        return wide_copy(4 + way, count, up if way else down)

    for layer in range(1):
        pltpu.make_async_copy(weights.at[layer], kernels.at[layer], local_sem.at[layer]).wait()

    @pl.when(core == 1)
    def _():
        for tap in range(9):
            wide[y, tap] = kernels[
                0, tap // 3, (tap % 3) * channels : (tap % 3 + 1) * channels
            ].astype(jnp.float32)
        for count in range(DIRECT):
            wide_copy(0, count, y).start()
            wide_copy(1, count, y).start()
        pltpu.make_async_copy(weights.at[0], coarse.at[y], local_sem.at[LAYERS]).start()

    def relax(layer, carry):
        center, inverse = statistics(gather_sums(layer))
        activate(state, SAMPLES, center, gains[pl.ds(layer, 1)] * inverse, offsets[pl.ds(layer, 1)])

        @pl.when(layer > 0)
        def _():
            pltpu.make_async_copy(weights.at[layer], kernels.at[layer], local_sem.at[layer]).wait()

        plain = square = jnp.zeros((8, channels), jnp.float32)
        for sample in range(SAMPLES):
            value = state[sample] + FINE * convolve(sample, lambda tap: kernels[layer, tap])
            state[sample] = value
            plain, square = plain + folded(value), square + folded(value * value)
        store_sums(layer + 1, plain, square)
        send_sums(layer + 1)
        return carry

    lax.fori_loop(0, LAYERS, relax, 0)

    following = {"z": next_z, "y": up}
    relaxed_copy = remote(state, begin, pass_send.at[0], pass_recv.at[0], following)

    @pl.when(position < final)
    def _():
        relaxed_copy.start()

    passed_sums[0] = gather_sums(LAYERS)
    totals_copy = remote(
        passed_sums.at[0], passed_sums.at[1], pass_send.at[1], pass_recv.at[1], following
    )

    @pl.when(position < final)
    def _():
        totals_copy.start()

    @pl.when(core == 1)
    def _():
        for count in range(DIRECT):
            wide_copy(0, count, down).wait_recv()
            wide_copy(2, count, down).start()
            wide_copy(1, count, up).wait_recv()
            if count < 9 - DIRECT:
                wide_copy(3, count, up).start()
            if count < SHARED // 2:
                pair_copy(0, count).start()
                pair_copy(1, count).start()

    @pl.when(position > 0)
    def _():
        totals_copy.wait_recv()
        relaxed_copy.wait_recv()

    @pl.when(position == 0)
    def _():
        first = sums[0, 0]
        for peer in range(1, peers):
            first = first + sums[0, peer]
        passed_sums[1] = first
        for sample in range(SAMPLES):
            begin[sample] = iterate[sample]

    center, inverse = statistics(passed_sums[1])
    gain, offset = gains[0:1] * inverse, offsets[0:1]
    params[y, 0:1] = center
    params[y, 1:2] = gain
    params[y, 2:3] = offset

    def param_copy(step, sender_step):
        return remote(
            params.at[y],
            params.at[y],
            param_send.at[step],
            param_recv.at[lax.rem(y + sender_step, COLUMN)],
            {"y": lax.rem(y + step, COLUMN), "core": 1},
        )

    @pl.when(core == 1)
    def _():
        for step in range(1, COLUMN):
            param_copy(step, 0).start()

    activate(begin, SAMPLES, center, gain, offset)

    @pl.when(position < final)
    def _():
        relaxed_copy.wait_send()

    plain = square = jnp.zeros((8, channels), jnp.float32)
    for sample in range(SAMPLES):
        increment = convolve(sample, lambda tap: kernels[0, tap])
        value = begin[sample]
        kept[sample] = value + COARSE * increment
        value = value + FINE * increment
        state[sample] = value
        plain, square = plain + folded(value), square + folded(value * value)
    store_sums(LAYERS + 1, plain, square)
    send_sums(LAYERS + 1)

    @pl.when(core == 1)
    def _():
        pair_copy(0, 2).start()

    def refine(layer, carry):
        center, inverse = statistics(gather_sums(LAYERS + layer))
        activate(state, SAMPLES, center, gains[pl.ds(layer, 1)] * inverse, offsets[pl.ds(layer, 1)])
        plain = square = jnp.zeros((8, channels), jnp.float32)
        for sample in range(SAMPLES):
            value = state[sample] + FINE * convolve(sample, lambda tap: kernels[layer, tap])
            state[sample] = value
            plain, square = plain + folded(value), square + folded(value * value)
        store_sums(LAYERS + layer + 1, plain, square)
        send_sums(LAYERS + layer + 1)

        @pl.when((core == 1) & (layer == 1))
        def _():
            pair_copy(1, 2).start()

        @pl.when((core == 1) & (layer == 2))
        def _():
            for way in range(2):
                pair_copy(way, 3).start()

        return carry

    lax.fori_loop(1, LAYERS - 1, refine, 0)

    def force_copy(sample):
        return remote(
            kept.at[sample],
            forcing.at[y],
            force_send.at[sample],
            force_recv.at[y],
            {"y": 2 * core + sample, "core": 1},
        )

    last = LAYERS - 1
    center, inverse = statistics(gather_sums(LAYERS + last))
    activate(state, SAMPLES, center, gains[last : last + 1] * inverse, offsets[last : last + 1])
    for sample in range(SAMPLES):
        value = state[sample] + FINE * convolve(sample, lambda tap: kernels[last, tap])
        value = value - kept[sample]
        kept[sample] = value
        here = (core == 1) & (y == 2 * core + sample)

        @pl.when(here)
        def _():
            forcing[y] = kept[sample]

        @pl.when(jnp.logical_not(here))
        def _():
            force_copy(sample).start()

    holder = y // 2
    slot = lax.rem(y, 2)

    def out_copy(block):
        return remote(
            chain.at[block + 1],
            out.at[slot],
            out_send.at[block],
            out_recv.at[slot],
            {"y": block, "core": holder},
        )

    def hop(part):
        return remote(
            chain.at[COLUMN, pl.ds(part * half, half)],
            chain.at[0, pl.ds(part * half, half)],
            chain_send.at[part],
            chain_recv.at[part],
            {"z": above, "core": 1},
        )

    def own_copy(block):
        return pltpu.make_async_copy(chain.at[block + 1], out.at[slot], local_sem.at[LAYERS + 1])

    @pl.when(core == 1)
    def _():
        for count in range(DIRECT):
            wide_copy(2, count, 0).wait_recv()
        for count in range(9 - DIRECT):
            wide_copy(3, count, 0).wait_recv()
        for count in range(SHARED):
            pair_copy(0, count).wait_recv()
            pair_copy(1, count).wait_recv()
        for step in range(1, COLUMN):
            origin = lax.rem(y + step, COLUMN)
            for tap in range(9):
                coarse[
                    origin, tap // 3, (tap % 3) * channels : (tap % 3 + 1) * channels
                ] = wide[origin, tap].astype(jnp.bfloat16)
            param_copy(step, step).wait_recv()
        pltpu.make_async_copy(weights.at[0], coarse.at[y], local_sem.at[LAYERS]).wait()
        for block in range(COLUMN):
            center, gain, offset = (params[block, row : row + 1] for row in range(3))
            source = chain.at[pl.ds(block, 1)]
            if block == 0:
                for part in range(HALVES):
                    hop(part).wait_recv()
                    activate(source, 1, center, gain, offset, range(part * half, part * half + half))
            else:
                activate(source, 1, center, gain, offset)

            @pl.when(jnp.logical_or(block != y, y < 2))
            def _():
                remote(
                    kept.at[0],
                    forcing.at[block],
                    force_send.at[0],
                    force_recv.at[block],
                    {"y": block, "core": 1},
                ).wait_recv()

            if block < COLUMN - 1:
                increment = convolve(0, lambda tap: coarse[block, tap])
                chain[block + 1] = chain[block] + COARSE * increment + forcing[block]
            else:
                for part in range(HALVES):
                    first = part * half
                    taken = pl.ds(first, half)
                    increment = convolve(0, lambda tap: coarse[block, tap], first, half)
                    chain[block + 1, taken] = (
                        chain[block, taken] + COARSE * increment + forcing[block, taken]
                    )

                    @pl.when(z < planes - 1)
                    def _():
                        hop(part).start()

            here = (y == block) & (holder == 1)

            @pl.when(here)
            def _():
                own_copy(block).start()

            @pl.when(jnp.logical_not(here))
            def _():
                out_copy(block).start()

        @pl.when(holder == 1)
        def _():
            own_copy(0).wait()

    for sample in range(SAMPLES):

        @pl.when(jnp.logical_not((core == 1) & (y == 2 + sample)))
        def _():
            remote(
                chain.at[1],
                out.at[sample],
                out_send.at[0],
                out_recv.at[sample],
                {"y": y, "core": core},
            ).wait_recv()

    for exchange in range(EXCHANGES):
        for step in range(1, peers):
            peer_copy(exchange, step, 0).wait_send()

    @pl.when(position < final)
    def _():
        totals_copy.wait_send()

    for sample in range(SAMPLES):

        @pl.when(position == 0)
        def _():
            for part in range(HALVES):
                start_copy(sample, part).wait_send()

        @pl.when(jnp.logical_not((core == 1) & (y == 2 * core + sample)))
        def _():
            force_copy(sample).wait_send()

    @pl.when(core == 1)
    def _():
        for count in range(DIRECT):
            wide_copy(0, count, y).wait_send()
            wide_copy(1, count, y).wait_send()
            wide_copy(2, count, down).wait_send()
        for count in range(9 - DIRECT):
            wide_copy(3, count, up).wait_send()
        for count in range(SHARED):
            pair_copy(0, count).wait_send()
            pair_copy(1, count).wait_send()
        for step in range(1, COLUMN):
            param_copy(step, 0).wait_send()
        for block in range(COLUMN):

            @pl.when(jnp.logical_not((y == block) & (holder == 1)))
            def _():
                out_copy(block).wait_send()

        @pl.when(z < planes - 1)
        def _():
            for part in range(HALVES):
                hop(part).wait_send()


def block_solve(planes, chips, iterate, weights, gains, offsets):
    _, samples, side, _, channels = iterate.shape
    state = (samples, side, side, channels)
    peers = chips * 2
    dma = pltpu.SemaphoreType.DMA
    result = pl.pallas_call(
        functools.partial(kernel, planes, chips),
        out_shape=jax.ShapeDtypeStruct(state, jnp.float32),
        in_specs=[
            pl.BlockSpec(memory_space=pltpu.VMEM),
            pl.BlockSpec(memory_space=pl.ANY),
            pl.BlockSpec(memory_space=pltpu.VMEM),
            pl.BlockSpec(memory_space=pltpu.VMEM),
        ],
        out_specs=pl.BlockSpec(memory_space=pl.ANY),
        scratch_shapes=[
            pltpu.VMEM(state, jnp.float32),
            pltpu.VMEM(state, jnp.float32),
            pltpu.VMEM(state, jnp.float32),
            pltpu.VMEM((LAYERS, 3, 3 * channels, channels), jnp.bfloat16),
            pltpu.VMEM((samples, side + 2, side, 3 * channels), jnp.bfloat16),
            pltpu.VMEM((EXCHANGES, peers, 2, channels), jnp.float32),
            pltpu.VMEM((2, 2, channels), jnp.float32),
            pltpu.VMEM((COLUMN, side, side, channels), jnp.float32),
            pltpu.VMEM((COLUMN + 1, side, side, channels), jnp.float32),
            pltpu.VMEM((COLUMN, 9, channels, channels), jnp.float32),
            pltpu.VMEM((COLUMN, 3, 3 * channels, channels), jnp.bfloat16),
            pltpu.VMEM((COLUMN, 8, channels), jnp.float32),
            dma((LAYERS + 2,)),
            dma((EXCHANGES, peers)),
            dma((EXCHANGES, peers)),
            dma((2,)),
            dma((2,)),
            dma((6, DIRECT)),
            dma((6, DIRECT)),
            dma((samples,)),
            dma((COLUMN,)),
            dma((COLUMN,)),
            dma((COLUMN,)),
            dma((samples, HALVES)),
            dma((HALVES,)),
            dma((HALVES,)),
            dma((COLUMN,)),
            dma((samples,)),
        ],
        compiler_params=pltpu.CompilerParams(
            collective_id=0, has_side_effects=True, vmem_limit_bytes=60 << 20
        ),
    )(
        iterate[0],
        weights.reshape(LAYERS, 3, 3 * channels, channels),
        gains,
        offsets,
    )
    return result[None]


def solution(mesh):
    planes = mesh.shape["depth"] // COLUMN
    chips = mesh.shape["batch"] // 2
    finer = Mesh(
        mesh.devices.reshape(planes, COLUMN, chips, 2), ("z", "y", "x", "core")
    )
    depth, batch = ("z", "y"), ("x", "core")
    return jax.shard_map(
        functools.partial(block_solve, planes, chips),
        mesh=finer,
        in_specs=(
            P(depth, batch, None, None, None),
            P(depth, None, None, None, None),
            P(depth, None),
            P(depth, None),
        ),
        out_specs=P(depth, batch, None, None, None),
        check_vma=False,
    )
```
